256 devices in a mesh: groups: 4 (over y, x), seq: 32 (over z), head: 2 (over core).
Axes of the slice: x: 2, y: 2, z: 32, core: 2. Of those that a mesh axis runs over, the one named last changes fastest.
The devices are a block of a 4x8x32 slice.
Arguments:
- q_latent: bfloat16 [128, 64, 512], P(('groups', 'seq'), 'head'), parts along dimension 0, may hold values from -7.5 to 7.5
- q_rope: bfloat16 [128, 4096], P(('groups', 'seq'), 'head'), parts along dimension 0, may hold values from -7.5 to 7.5
- cache_latent: bfloat16 [24576, 64, 512], P(('groups', 'seq', 'head')), parts along dimension 0, may hold values from -10 to 10
- cache_rope: bfloat16 [24576, 4096], P(('groups', 'seq', 'head')), parts along dimension 0, may hold values from -6 to 6
- page_table: int32 [128, 192], P('groups'), parts along dimension 0, may hold values from 0 to 6143, as said below
- lengths: int32 [128], P('groups'), parts along dimension 0, may hold values from 1 to 12288, 235929 in all
Outputs:
- attended: bfloat16 [128, 64, 512], P(('groups', 'seq'), 'head'), parts along dimension 0
The draws below stay inside these ranges and needn't reach their ends.
There are 4 independent parts, one for each index of `groups`. The reference program is written for one: setup_inputs(seed, part) draws one part's arguments, and reference() takes and returns one part's arrays. A program takes and returns all parts, laid end to end along the dimension named above; each array names one. Nothing has to cross between parts.
Inputs may be any that keep to these rules, and one draw needn't show every extreme that they name: `page_table`: device d of a group (d = seq index * 2 + head index) holds pool pages d * 96 to (d + 1) * 96 - 1. Each pool page is named exactly once. A request's logical pages k * 3 to (k + 1) * 3 - 1 lie on one device, and every device holds exactly one such run of every request. `lengths`: the newest token is counted.
All inputs are finite; a program needn't handle non-finite values.
Results may differ from the reference program's by a relative error of at most 0.0055.
Values may be sent and summed in bfloat16 or wider, within the bound.
No kernel may reach another device: no remote copies, remote signals or barrier semaphores. Data moves between devices by JAX's collectives and lax.ppermute only.
A program may use at most 128 MiB of HBM per device.

```python
import math
import jax
import jax.numpy as jnp
import numpy as np
from jax import lax

H = 64
LAT = 512
ROPE = 64
NOPE = 128
PAGE = 64
RUN = 3
REQS = 32
DEVS = 64
POOL_DEV = 96
POOL = 6144
MAXP = 192
CTX = 12288


def draw_q_latent(key, part):
    base_draw = 1.5 * jnp.clip(jax.random.normal(jax.random.fold_in(key, 5), (REQS, H, LAT), jnp.float32), -5.0, 5.0)
    return base_draw.astype(jnp.bfloat16)


def draw_cache_latent(key, part):
    base_draw = jnp.clip(jax.random.normal(jax.random.fold_in(key, 7), (POOL, PAGE, LAT), jnp.float32), -5.0, 5.0)
    return base_draw.astype(jnp.bfloat16)


def draw_page_table(key, part):
    owner_key, slot_key = jax.random.split(jax.random.fold_in(key, 11))
    owner_keys = jax.random.split(owner_key, REQS)
    run_owners = jax.vmap(lambda single: jax.random.permutation(single, DEVS))(owner_keys).astype(jnp.int32)
    slot_keys = jax.random.split(slot_key, DEVS)
    slot_perm = jax.vmap(lambda single: jax.random.permutation(single, POOL_DEV))(slot_keys).astype(jnp.int32)
    run_ids = jnp.arange(RUN, dtype=jnp.int32)
    req_ids = jnp.arange(REQS, dtype=jnp.int32)
    local_slot = slot_perm[run_owners[:, :, None], req_ids[:, None, None] * RUN + run_ids[None, None, :]]
    page_ids = run_owners[:, :, None] * POOL_DEV + local_slot
    return page_ids.reshape(REQS, MAXP).astype(jnp.int32)


def block_levels(key, extent, pieces, low, largest):
    factor_of, own = 1.0, jax.random.fold_in(key, 6)
    for dim, parts in pieces:
        draws = jnp.exp(jax.random.uniform(jax.random.fold_in(own, dim), (parts,), jnp.float32, low / len(pieces), largest / len(pieces)))
        factor_of = factor_of * jnp.repeat(draws, extent[dim] // parts).reshape([-1 if axis == dim else 1 for axis in range(len(extent))])
    return factor_of


def split_up(number_of, total, most, skew):
    portions = [(1 << 20) // math.isqrt(standing ** skew) + 1 for standing in range(2, number_of + 1)]
    rest, holding = total - most - (number_of - 1), [1] * (number_of - 1)
    while rest > 0:
        free = [i for i in range(number_of - 1) if holding[i] < most]
        pool, budget = sum([portions[i] for i in free]), rest
        for i in free:
            more = min(most - holding[i], max(1, budget * portions[i] // pool), rest)
            holding[i] = holding[i] + more
            rest = rest - more
    return np.array([most] + holding)


def uneven(key, number_of, total, limit, lean):
    if number_of == 2:
        one = jax.random.randint(key, (), max(1, total - limit), min(limit, total - 1) + 1)
        return jnp.stack([one, total - one])
    sizes = jnp.asarray(split_up(number_of, total, limit, lean), jnp.int32)
    pairs = (number_of - 1) // 2
    source_of, receiver = sizes[1:1 + 2 * pairs:2], sizes[2:2 + 2 * pairs:2]
    room = jnp.minimum(source_of - 1, limit - receiver)
    moved = jax.random.randint(jax.random.fold_in(key, 1), (pairs,), 0, 1 << 20) % (room + 1)
    sizes = sizes.at[1:1 + 2 * pairs:2].set(source_of - moved).at[2:2 + 2 * pairs:2].set(receiver + moved)
    return sizes[jax.random.permutation(jax.random.fold_in(key, 2), number_of)]


def scatter_about(own_key, extent, deviation, most, pieces=(), held_as=jnp.bfloat16):
    values = jax.random.normal(own_key, extent, jnp.float32) * deviation
    if len(pieces) > 0:
        values = block_levels(own_key, extent, pieces, -0.22, 0.18) * values
    return jnp.clip(values, min=-most, max=most).astype(held_as)


def setup_inputs(seed: int = 0, part: int = 0) -> dict:
    seeds = jax.random.split(jax.random.key(seed), 7)
    part_splits = jax.random.split(jax.random.fold_in(seeds[6], part), 7)
    q_latent = draw_q_latent(jax.random.fold_in(jax.random.fold_in(seeds[6], part), 71), part)
    q_rope = scatter_about(part_splits[1], (REQS, H * ROPE), 1.5, 7.5, ((0, 32), (1, 2)))
    cache_latent = draw_cache_latent(jax.random.fold_in(jax.random.fold_in(seeds[6], part), 71), part)
    cache_rope = scatter_about(part_splits[3], (POOL, PAGE * ROPE), 1.0, 6.0, ((0, 64),))
    page_table = draw_page_table(jax.random.fold_in(jax.random.fold_in(seeds[6], part), 71), part)
    lengths = uneven(part_splits[5], REQS, REQS * CTX * 3 // 5, CTX, 2).astype(jnp.int32)
    return dict(q_latent=q_latent, q_rope=q_rope, cache_latent=cache_latent, cache_rope=cache_rope, page_table=page_table, lengths=lengths)


MASKED_SCORE = -1e+30

def reference(q_latent, q_rope, cache_latent, cache_rope, page_table, lengths):
    score_scale = 1.0 / math.sqrt(NOPE + ROPE)
    positions = jnp.arange(MAXP * PAGE, dtype=jnp.int32)

    def attend_one(inputs_row):
        query_lat, query_rot, page_ids, seq_len = inputs_row
        key_rows = cache_latent[page_ids].reshape(MAXP * PAGE, LAT)
        rotary = cache_rope[page_ids].reshape(MAXP * PAGE, ROPE)
        scores = jnp.dot(query_lat, key_rows.T, preferred_element_type=jnp.float32)
        scores = scores + jnp.dot(query_rot.reshape(H, ROPE), rotary.T, preferred_element_type=jnp.float32)
        scores = scores * score_scale
        live_mask = positions < seq_len
        scores = jnp.where(live_mask[None, :], scores, MASKED_SCORE)
        row_max = lax.optimization_barrier(jnp.max(scores, axis=1, keepdims=True))
        exp_terms = jnp.where(live_mask[None, :], jnp.exp(scores - row_max), 0.0)
        row_total = lax.optimization_barrier(jnp.sum(exp_terms, axis=1, keepdims=True))
        weights = exp_terms.astype(jnp.bfloat16)
        summed = jnp.dot(weights, key_rows, preferred_element_type=jnp.float32)
        return (summed / row_total).astype(jnp.bfloat16)
    return lax.map(attend_one, (q_latent, q_rope, page_table, lengths))
```

```python
import math

import jax
import jax.numpy as jnp
from jax import lax
from jax.experimental import pallas as pl
from jax.experimental.pallas import tpu as pltpu
from jax.sharding import PartitionSpec as P

ROPE = 64
NOPE = 128
LANES = 128
STAT_ROWS = 16
MASKED_SCORE = -1e30


def shift_from(array, offset, axis):
    count = lax.axis_size(axis)
    return lax.ppermute(array, axis, [((i + offset) % count, i) for i in range(count)])


def gathered_by_offset(block, axis):
    count = lax.axis_size(axis)
    far, mid = 11, 4
    assert count == 32
    first = [(0, block)]
    for step in (far, -far):
        first.append((step, shift_from(block, step, axis)))
    three = jnp.concatenate([b for _, b in first], axis=0)
    base = [o for o, _ in first]
    pieces, offsets = [three], list(base)
    for step in (mid, -mid):
        pieces.append(shift_from(three, step, axis))
        offsets += [o + step for o in base]
    nine = jnp.concatenate(pieces, axis=0)
    place = {o: i for i, o in enumerate(offsets)}
    plus = shift_from(nine, 1, axis)
    minus = shift_from(nine, -1, axis)
    skip_plus = jnp.concatenate([nine[place[o] : place[o] + 1] for o in (0, 7, 11)], axis=0)
    skip_minus = jnp.concatenate([nine[place[o] : place[o] + 1] for o in (0, -7, -11)], axis=0)
    plus_two = shift_from(skip_plus, 2, axis)
    minus_two = shift_from(skip_minus, -2, axis)
    parts = [nine, plus, minus, plus_two, minus_two]
    listed = list(offsets) + [o + 1 for o in offsets] + [o - 1 for o in offsets]
    listed += [2, 9, 13, -2, -9, -13]
    return parts, listed


def attention_kernel(
    run_len, request_ref, own_ref, partner_ref, own_live_ref, partner_live_ref, q_ref, *refs
):
    latents, ropes, out_ref = refs[: 2 * run_len], refs[2 * run_len : 4 * run_len], refs[-1]
    step = pl.program_id(0)
    own_live, partner_live = own_live_ref[step], partner_live_ref[step]
    packed = q_ref.shape[1] - STAT_ROWS
    page_len, width = latents[0].shape[1:]
    slabs = width // LANES
    heads = packed // slabs
    half = run_len * page_len

    def store_stats(shift, total):
        lane = lax.broadcasted_iota(jnp.int32, (heads, LANES), 1)
        high = total.astype(jnp.bfloat16).astype(jnp.float32)
        stats = jnp.where(lane == 0, shift, jnp.where(lane == 1, high, total - high))
        turned = stats.T[:STAT_ROWS].astype(jnp.bfloat16)
        out_ref[0, packed:, :heads] = turned

    @pl.when(own_live + partner_live > 0)
    def _():
        block = q_ref[0]
        query = jnp.concatenate(
            [block[c * heads : (c + 1) * heads] for c in range(slabs)], axis=1
        )
        rope = block[packed:]
        lane = lax.broadcasted_iota(jnp.int32, rope.shape, 1)
        zero = jnp.zeros_like(rope)
        query_rope = jnp.concatenate(
            [jnp.where(lane < ROPE, rope, zero), jnp.where(lane >= ROPE, rope, zero)], axis=0
        )
        keys = jnp.concatenate([ref[0] for ref in latents], axis=0)
        rotary = jnp.concatenate([ref[0] for ref in ropes], axis=0)
        over_width = (((1,), (1,)), ((), ()))
        scores = lax.dot_general(query, keys, over_width, preferred_element_type=jnp.float32)
        scores = scores + lax.dot_general(
            query_rope, rotary, over_width, preferred_element_type=jnp.float32
        )
        scores = scores * (1.0 / math.sqrt(NOPE + ROPE))
        column = lax.broadcasted_iota(jnp.int32, scores.shape, 1)
        live = column < jnp.where(column < half, own_live, half + partner_live)
        scores = jnp.where(live, scores, MASKED_SCORE)
        shift = jnp.max(scores, axis=1, keepdims=True)
        shift = shift.astype(jnp.bfloat16).astype(jnp.float32)
        probs = jnp.where(live, jnp.exp(scores - shift), 0.0)
        total = jnp.sum(probs, axis=1, keepdims=True)
        summed = jnp.dot(probs.astype(jnp.bfloat16), keys, preferred_element_type=jnp.float32)
        summed = summed.astype(jnp.bfloat16)
        for c in range(slabs):
            out_ref[0, c * heads : (c + 1) * heads, :] = summed[:, c * LANES : (c + 1) * LANES]
        store_stats(shift, total)

    @pl.when(own_live + partner_live == 0)
    def _():
        out_ref[0, :packed, :] = jnp.zeros((packed, LANES), out_ref.dtype)
        store_stats(
            jnp.full((heads, 1), MASKED_SCORE, jnp.float32), jnp.zeros((heads, 1), jnp.float32)
        )


def attention(tables, queries, own_lat, partner_lat, own_rot, partner_rot, run_len):
    steps, rows, _ = queries.shape
    page_len, width = own_lat.shape[1:]

    def page_spec(array, which, j):
        def index(step, request, own, partner, own_live, partner_live):
            return ((own, partner)[which][step * run_len + j], 0, 0)

        return pl.BlockSpec((1,) + array.shape[1:], index)

    both_lat, both_rot = (own_lat, partner_lat), (own_rot, partner_rot)
    specs = [pl.BlockSpec((1, rows, LANES), lambda step, *_: (step, 0, 0))]
    operands = [queries]
    for both in (both_lat, both_rot):
        for which in range(2):
            for j in range(run_len):
                specs.append(page_spec(both[which], which, j))
                operands.append(both[which])
    tokens = 2 * run_len * page_len
    heads = (rows - STAT_ROWS) * LANES // width
    return pl.pallas_call(
        lambda *refs: attention_kernel(run_len, *refs),
        out_shape=jax.ShapeDtypeStruct((steps, rows, LANES), jnp.bfloat16),
        grid_spec=pltpu.PrefetchScalarGridSpec(
            num_scalar_prefetch=len(tables),
            grid=(steps,),
            in_specs=specs,
            out_specs=pl.BlockSpec(
                (1, rows, LANES), lambda step, request, *_: (request[step], 0, 0)
            ),
        ),
        cost_estimate=pl.CostEstimate(
            flops=steps * tokens * heads * (4 * width + 4 * ROPE),
            bytes_accessed=steps * tokens * (width + LANES) * 2,
            transcendentals=steps * tokens * heads,
        ),
        name="attention",
    )(*tables, *operands)


def local(q_latent, q_rope, cache_latent, cache_rope, page_table, lengths):
    seq_count = lax.axis_size("seq")
    head_count = lax.axis_size("head")
    my_seq = lax.axis_index("seq")
    my_core = lax.axis_index("head")
    pool_pages, page_len, latent_width = cache_latent.shape
    rope_width = cache_rope.shape[1] // page_len
    request_count, page_slots = page_table.shape
    device_count = seq_count * head_count
    run_len = page_slots // device_count
    heads = q_latent.shape[1]
    slabs = latent_width // LANES

    slab_rows = [q_latent[0, :, c * LANES : (c + 1) * LANES] for c in range(slabs)]
    rope_rows = q_rope.reshape(2, heads // 2, rope_width)
    rope_rows = jnp.concatenate([rope_rows[0], rope_rows[1]], axis=1)
    block = jnp.concatenate(slab_rows + [rope_rows], axis=0)[None]

    swap = [(i, head_count - 1 - i) for i in range(head_count)]
    partner_lat = lax.ppermute(cache_latent, "head", swap)
    own_rot = cache_rope.reshape(pool_pages, page_len, rope_width)
    own_rot = jnp.concatenate([own_rot, own_rot], axis=2)
    partner_rot = lax.ppermute(own_rot, "head", swap)

    parts, offsets = gathered_by_offset(block, "seq")
    seen, keep = set(), []
    for i, o in enumerate(offsets):
        if o % seq_count not in seen:
            seen.add(o % seq_count)
            keep.append(i)
    queries = jnp.concatenate(parts, axis=0)
    if len(keep) < len(offsets):
        dropped = [i for i in range(len(offsets)) if i not in keep]
        pieces, at = [], 0
        for d in dropped + [len(offsets)]:
            pieces.append(queries[at:d])
            at = d + 1
        queries = jnp.concatenate(pieces, axis=0)
    kept = jnp.array([offsets[i] % seq_count for i in keep], jnp.int32)
    request = (my_seq + kept) % seq_count

    run_owner = page_table[:, ::run_len] // pool_pages
    run_ids = jnp.arange(device_count, dtype=jnp.int32)
    slots = page_table.reshape(request_count, device_count, run_len)

    def runs_on(device):
        here = run_owner == device
        run_index = jnp.sum(jnp.where(here, run_ids[None, :], 0), axis=1)
        pages = jnp.sum(jnp.where(here[:, :, None], slots, 0), axis=1) - device * pool_pages
        live = jnp.clip(lengths - run_index * run_len * page_len, 0, run_len * page_len)
        return pages[request].reshape(-1), live[request]

    own_pages, own_live = runs_on(my_seq * head_count + my_core)
    partner_pages, partner_live = runs_on(my_seq * head_count + head_count - 1 - my_core)

    partial = attention(
        (request, own_pages, partner_pages, own_live, partner_live),
        queries, cache_latent, partner_lat, own_rot, partner_rot, run_len,
    )
    got = lax.all_to_all(partial, "seq", split_axis=0, concat_axis=0, tiled=True)

    packed = slabs * heads
    stats = got[:, packed:, :heads].astype(jnp.float32)
    got_max = stats[:, 0]
    got_total = stats[:, 1] + stats[:, 2]
    shrink = jnp.exp(got_max - jnp.max(got_max, axis=0)[None])
    merged_total = jnp.sum(got_total * shrink, axis=0)
    got_sum = got[:, :packed].reshape(seq_count, slabs, heads, LANES).astype(jnp.float32)
    merged_sum = jnp.sum(got_sum * shrink[:, None, :, None], axis=0)
    merged = merged_sum / merged_total[None, :, None]
    merged = jnp.concatenate([merged[c] for c in range(slabs)], axis=1)
    return merged.astype(jnp.bfloat16)[None]


def solution(mesh):
    return jax.shard_map(
        local,
        mesh=mesh,
        in_specs=(
            P(("groups", "seq"), "head", None),
            P(("groups", "seq"), "head"),
            P(("groups", "seq", "head"), None, None),
            P(("groups", "seq", "head"), None),
            P("groups", None),
            P("groups"),
        ),
        out_specs=P(("groups", "seq"), "head", None),
        check_vma=False,
    )
```

```python
import math

import jax
import jax.numpy as jnp
from jax import lax
from jax.experimental import pallas as pl
from jax.experimental.pallas import tpu as pltpu
from jax.sharding import PartitionSpec as P

ROPE = 64
NOPE = 128
LANES = 128
STAT_ROWS = 16
MASKED_SCORE = -1e30

FAR = (0, 6, 13, -13, -6)
NEAR = {
    1: FAR,
    -1: FAR,
    2: FAR,
    -2: FAR,
    3: (0, 6, 13, -13),
    -3: (0, 13, -6),
}

VMEM = pl.BlockSpec(memory_space=pltpu.VMEM)
HBM = pl.BlockSpec(memory_space=pltpu.HBM)
LIMIT = pltpu.CompilerParams(vmem_limit_bytes=12 << 20)
ATTENTION_LIMIT = pltpu.CompilerParams(vmem_limit_bytes=50 << 20)


def shift_from(array, offset, axis):
    count = lax.axis_size(axis)
    return lax.ppermute(array, axis, [((i + offset) % count, i) for i in range(count)])


def parts_of(x, count):
    parts = []
    for _ in range(count - 1):
        high = x.astype(jnp.bfloat16).astype(jnp.float32)
        parts.append(high)
        x = x - high
    return parts + [x]


def pack_kernel(q_ref, rope_ref, out_ref):
    heads, width = q_ref.shape[1:]
    for c in range(width // LANES):
        out_ref[0, c * heads : (c + 1) * heads, :] = q_ref[0, :, c * LANES : (c + 1) * LANES]
    out_ref[0, heads * width // LANES :, :] = rope_ref[...]


def attention_kernel(offsets, run_len, count, table_ref, q_ref, *refs):
    caches, (out_ref, lat_buf, rot_buf, sems) = refs[:4], refs[4:]
    own_lat, partner_lat, own_rot, partner_rot = caches
    page_len, width = own_lat.shape[1:]
    packed = q_ref.shape[1] - STAT_ROWS
    slabs = width // LANES
    heads = packed // slabs
    half = run_len * page_len
    entry = 2 * (run_len + 1)
    me = table_ref[count * entry]

    def copies(g):
        request = lax.rem(me + offsets[g] % count, count)
        made = []
        for which in range(2):
            for j in range(run_len):
                page = table_ref[request * entry + which * (run_len + 1) + j]
                slot = which * run_len + j
                rows = pl.ds(slot * page_len, page_len)
                for kind, (source, buf) in enumerate(
                    (((own_lat, partner_lat)[which], lat_buf), ((own_rot, partner_rot)[which], rot_buf))
                ):
                    made.append(
                        pltpu.make_async_copy(
                            source.at[page], buf.at[g, rows], sems.at[g, 2 * slot + kind]
                        )
                    )
        return request, made

    started = []
    for g in range(len(offsets)):
        request, made = copies(g)
        for copy in made:
            copy.start()
        started.append((request, made))

    lane = lax.broadcasted_iota(jnp.int32, (heads, LANES), 1)
    rope_lane = lax.broadcasted_iota(jnp.int32, (STAT_ROWS, LANES), 1)
    column = lax.broadcasted_iota(jnp.int32, (heads, 2 * half), 1)
    over_width = (((1,), (1,)), ((), ()))
    for g in range(len(offsets)):
        request, made = started[g]
        own_live = table_ref[request * entry + run_len]
        partner_live = table_ref[request * entry + 2 * run_len + 1]
        query = jnp.concatenate(
            [q_ref[g, c * heads : (c + 1) * heads, :] for c in range(slabs)], axis=1
        )
        rope = q_ref[g, packed:, :]
        zero = jnp.zeros_like(rope)
        query_rope = jnp.concatenate(
            [jnp.where(rope_lane < ROPE, rope, zero), jnp.where(rope_lane >= ROPE, rope, zero)],
            axis=0,
        )
        for copy in made:
            copy.wait()
        keys, rotary = lat_buf[g], rot_buf[g]
        scores = lax.dot_general(query, keys, over_width, preferred_element_type=jnp.float32)
        scores = scores + lax.dot_general(
            query_rope, rotary, over_width, preferred_element_type=jnp.float32
        )
        scores = scores * (1.0 / math.sqrt(NOPE + ROPE))
        live = column < jnp.where(column < half, own_live, half + partner_live)
        scores = jnp.where(live, scores, MASKED_SCORE)
        top = jnp.max(scores, axis=1, keepdims=True)
        probs = jnp.where(live, jnp.exp(scores - top), 0.0)
        total = jnp.sum(probs, axis=1, keepdims=True)
        summed = jnp.dot(probs.astype(jnp.bfloat16), keys, preferred_element_type=jnp.float32)
        summed = summed.astype(jnp.bfloat16)
        for c in range(slabs):
            out_ref[g, c * heads : (c + 1) * heads, :] = summed[:, c * LANES : (c + 1) * LANES]
        stats = jnp.zeros((heads, LANES), jnp.float32)
        for i, part in enumerate(parts_of(top, 3) + parts_of(total, 2)):
            stats = jnp.where(lane == i, part, stats)
        out_ref[g, packed:, :] = jnp.zeros((STAT_ROWS, LANES), out_ref.dtype)
        out_ref[g, packed:, :heads] = stats.T[:STAT_ROWS].astype(out_ref.dtype)


def attention(offsets, table, queries, caches, run_len, count):
    groups, rows, _ = queries.shape
    page_len, width = caches[0].shape[1:]
    tokens = 2 * run_len * page_len
    heads = (rows - STAT_ROWS) * LANES // width
    work = groups * tokens
    return pl.pallas_call(
        lambda *refs: attention_kernel(offsets, run_len, count, *refs),
        out_shape=jax.ShapeDtypeStruct((groups, rows, LANES), jnp.bfloat16),
        in_specs=[pl.BlockSpec(memory_space=pltpu.SMEM), VMEM] + [HBM] * 4,
        out_specs=VMEM,
        scratch_shapes=[
            pltpu.VMEM((groups, tokens, width), jnp.bfloat16),
            pltpu.VMEM((groups, tokens, LANES), jnp.bfloat16),
            pltpu.SemaphoreType.DMA((groups, 4 * run_len)),
        ],
        cost_estimate=pl.CostEstimate(
            flops=work * heads * (4 * width + 4 * ROPE),
            bytes_accessed=work * (width + LANES) * 2,
            transcendentals=work * heads,
        ),
        compiler_params=ATTENTION_LIMIT,
        name="attention",
    )(table, queries, *caches)


def merge_blocks(blocks, packed, heads, final):
    rows = [ref[i, packed:, :].astype(jnp.float32) for ref, i in blocks]
    tops = [r[0:1] + r[1:2] + r[2:3] for r in rows]
    totals = [r[3:4] + r[4:5] for r in rows]
    best = tops[0]
    for top in tops[1:]:
        best = jnp.maximum(best, top)
    weights = [jnp.exp(top - best) for top in tops]
    total = sum(w * t for w, t in zip(weights, totals))
    if final:
        weights = [w / total for w in weights]
    padded = weights + [jnp.zeros_like(best)] * (8 - len(weights))
    columns = jnp.concatenate(padded, axis=0).T
    columns = [columns[:heads, k : k + 1] for k in range(len(blocks))]
    slabs = []
    for c in range(packed // heads):
        slab = 0.0
        for column, (ref, i) in zip(columns, blocks):
            slab += column * ref[i, c * heads : (c + 1) * heads, :].astype(jnp.float32)
        slabs.append(slab.astype(jnp.bfloat16))
    if final:
        return slabs, None
    stats = parts_of(best, 3) + parts_of(total, 2)
    stats += [jnp.zeros((STAT_ROWS - len(stats), LANES), jnp.float32)]
    return slabs, jnp.concatenate(stats, axis=0).astype(jnp.bfloat16)


def near_merge_kernel(heads, sources, *refs):
    inputs, outs = refs[: len(sources)], refs[len(sources) :]
    packed = outs[0].shape[1] - STAT_ROWS
    for o, out_ref in zip(FAR, outs):
        blocks = [(ref, held.index(o)) for ref, held in zip(inputs, sources) if o in held]
        slabs, stats = merge_blocks(blocks, packed, heads, False)
        for c, slab in enumerate(slabs):
            out_ref[0, c * heads : (c + 1) * heads, :] = slab
        out_ref[0, packed:, :] = stats


def far_merge_kernel(*refs):
    inputs, out_ref = refs[:-1], refs[-1]
    heads = out_ref.shape[1]
    packed = inputs[0].shape[1] - STAT_ROWS
    slabs, _ = merge_blocks([(ref, 0) for ref in inputs], packed, heads, True)
    for c, slab in enumerate(slabs):
        out_ref[0, :, c * LANES : (c + 1) * LANES] = slab


def local(q_latent, q_rope, cache_latent, cache_rope, page_table, lengths):
    seq_count = lax.axis_size("seq")
    head_count = lax.axis_size("head")
    my_seq = lax.axis_index("seq")
    my_core = lax.axis_index("head")
    pool_pages, page_len, latent_width = cache_latent.shape
    rope_width = cache_rope.shape[1] // page_len
    request_count, page_slots = page_table.shape
    device_count = seq_count * head_count
    run_len = page_slots // device_count
    heads = q_latent.shape[1]
    reached = {o % seq_count for o in FAR} | {(o + d) % seq_count for d in NEAR for o in NEAR[d]}
    assert len(reached) == seq_count == len(FAR) + sum(len(held) for held in NEAR.values())

    rope_rows = q_rope.reshape(2, heads // 2, rope_width)
    rope_rows = jnp.concatenate([rope_rows[0], rope_rows[1]], axis=1)
    block_shape = (1, heads * latent_width // LANES + STAT_ROWS, LANES)
    block = pl.pallas_call(
        pack_kernel,
        out_shape=jax.ShapeDtypeStruct(block_shape, jnp.bfloat16),
        in_specs=[VMEM] * 2,
        out_specs=VMEM,
        compiler_params=LIMIT,
        name="pack",
    )(q_latent, rope_rows)

    swap = [(i, head_count - 1 - i) for i in range(head_count)]
    partner_lat = lax.ppermute(cache_latent, "head", swap)
    own_rot = cache_rope.reshape(pool_pages, page_len, rope_width)
    own_rot = jnp.concatenate([own_rot, own_rot], axis=2)
    partner_rot = lax.ppermute(own_rot, "head", swap)
    caches = (cache_latent, partner_lat, own_rot, partner_rot)

    run_owner = page_table[:, ::run_len] // pool_pages
    run_ids = jnp.arange(device_count, dtype=jnp.int32)
    slots = page_table.reshape(request_count, device_count, run_len)

    def runs_on(device):
        here = run_owner == device
        run_index = jnp.sum(jnp.where(here, run_ids[None, :], 0), axis=1)
        pages = jnp.sum(jnp.where(here[:, :, None], slots, 0), axis=1) - device * pool_pages
        live = jnp.clip(lengths - run_index * run_len * page_len, 0, run_len * page_len)
        return [pages, live[:, None]]

    entries = runs_on(my_seq * head_count + my_core)
    entries += runs_on(my_seq * head_count + head_count - 1 - my_core)
    table = jnp.concatenate(entries, axis=1).astype(jnp.int32).reshape(-1)
    table = jnp.concatenate([table, my_seq.astype(jnp.int32)[None]])

    def attend(offsets, queries):
        return attention(offsets, table, queries, caches, run_len, seq_count)

    far_blocks = [block if o == 0 else shift_from(block, o, "seq") for o in FAR]
    far = jnp.concatenate(far_blocks, axis=0)

    def chosen(held):
        return far if held == FAR else jnp.concatenate([far_blocks[FAR.index(o)] for o in held])

    near = {d: shift_from(chosen(held), d, "seq") for d, held in NEAR.items()}
    partials, sources = [attend(FAR, far)], [FAR]
    for d, held in NEAR.items():
        partial = attend(tuple(o + d for o in held), near[d])
        partials.append(shift_from(partial, -d, "seq"))
        sources.append(held)

    merged = pl.pallas_call(
        lambda *refs: near_merge_kernel(heads, sources, *refs),
        out_shape=[jax.ShapeDtypeStruct(block_shape, jnp.bfloat16)] * len(FAR),
        in_specs=[VMEM] * len(sources),
        out_specs=[VMEM] * len(FAR),
        compiler_params=LIMIT,
        name="near_merge",
    )(*partials)
    arrived = [b if o == 0 else shift_from(b, -o, "seq") for o, b in zip(FAR, merged)]
    return pl.pallas_call(
        far_merge_kernel,
        out_shape=jax.ShapeDtypeStruct((1, heads, latent_width), jnp.bfloat16),
        in_specs=[VMEM] * len(arrived),
        out_specs=VMEM,
        compiler_params=LIMIT,
        name="far_merge",
    )(*arrived)


def solution(mesh):
    return jax.shard_map(
        local,
        mesh=mesh,
        in_specs=(
            P(("groups", "seq"), "head", None),
            P(("groups", "seq"), "head"),
            P(("groups", "seq", "head"), None, None),
            P(("groups", "seq", "head"), None),
            P("groups", None),
            P("groups"),
        ),
        out_specs=P(("groups", "seq"), "head", None),
        check_vma=False,
    )
```

```python
import math

import jax
import jax.numpy as jnp
from jax import lax
from jax.experimental import pallas as pl
from jax.experimental.pallas import tpu as pltpu
from jax.sharding import PartitionSpec as P

ROPE = 64
NOPE = 128
LANES = 128
STAT_ROWS = 16
MASKED_SCORE = -1e30

FAR = (0, 6, 13, -6, -13)
NEAR = {
    1: FAR,
    -1: FAR,
    2: FAR,
    -2: FAR,
    3: (0, 6, 13, -13),
    -3: (0, 13, -6),
}
GROUPS = ((0, FAR),) + tuple(NEAR.items())

VMEM = pl.BlockSpec(memory_space=pltpu.VMEM)
HBM = pl.BlockSpec(memory_space=pltpu.HBM)
LIMIT = pltpu.CompilerParams(vmem_limit_bytes=12 << 20)


def shift_from(array, offset):
    count, cores = lax.axis_size("seq"), lax.axis_size("head")
    pairs = [
        (((i + (1 - 2 * c) * offset) % count) * cores + c, i * cores + c)
        for i in range(count)
        for c in range(cores)
    ]
    return lax.ppermute(array, ("seq", "head"), pairs)


def swapped(array):
    cores = lax.axis_size("head")
    return lax.ppermute(array, "head", [(c, cores - 1 - c) for c in range(cores)])


def joined(name, arrays, *picks):
    def kernel(*refs):
        for out_ref, pick in zip(refs[len(arrays) :], picks):
            for at, (k, i) in enumerate(pick):
                out_ref[at] = refs[k][i]

    shape = arrays[0].shape[1:]
    outs = pl.pallas_call(
        kernel,
        out_shape=[jax.ShapeDtypeStruct((len(p),) + shape, arrays[0].dtype) for p in picks],
        in_specs=[VMEM] * len(arrays),
        out_specs=[VMEM] * len(picks),
        compiler_params=LIMIT,
        name=name,
    )(*arrays)
    return outs[0] if len(picks) == 1 else outs


def parts_of(x, count):
    parts = []
    for _ in range(count - 1):
        high = x.astype(jnp.bfloat16).astype(jnp.float32)
        parts.append(high)
        x = x - high
    return parts + [x]


def pack_kernel(q_ref, rope_ref, out_ref):
    heads, width = q_ref.shape[1:]
    for c in range(width // LANES):
        out_ref[0, c * heads : (c + 1) * heads, :] = q_ref[0, :, c * LANES : (c + 1) * LANES]
    out_ref[0, heads * width // LANES :, :] = rope_ref[...]


def request_at(table_ref, offset, count):
    return lax.rem(table_ref[0] + table_ref[1] * offset + count, count)


def gather_kernel(run_len, count, table_ref, own_lat, partner_lat, own_rot, partner_rot, *refs):
    outs, sems = refs[:-1], refs[-1]
    page_len = own_lat.shape[1]
    entry = 2 * (run_len + 1)
    for k, (d, held) in enumerate(GROUPS):
        keys_ref, rotary_ref = outs[2 * k], outs[2 * k + 1]
        for g, o in enumerate(held):
            request = request_at(table_ref, o + d, count)
            for which, (lat, rot) in enumerate(((own_lat, own_rot), (partner_lat, partner_rot))):
                for j in range(run_len):
                    page = table_ref[2 + request * entry + which * (run_len + 1) + j]
                    rows = pl.ds((which * run_len + j) * page_len, page_len)
                    pltpu.make_async_copy(lat.at[page], keys_ref.at[g, rows], sems.at[2 * k]).start()
                    pltpu.make_async_copy(
                        rot.at[page], rotary_ref.at[g, rows], sems.at[2 * k + 1]
                    ).start()
    for k, ref in enumerate(outs):
        pltpu.make_async_copy(ref, ref, sems.at[k]).wait()


def gather_pages(table, caches, run_len, count):
    page_len, width = caches[0].shape[1:]
    tokens = 2 * run_len * page_len
    shapes = []
    for _, held in GROUPS:
        for lanes in (width, LANES):
            shapes.append(jax.ShapeDtypeStruct((len(held), tokens, lanes), jnp.bfloat16))
    outs = pl.pallas_call(
        lambda *refs: gather_kernel(run_len, count, *refs),
        out_shape=shapes,
        in_specs=[pl.BlockSpec(memory_space=pltpu.SMEM)] + [HBM] * 4,
        out_specs=[VMEM] * len(shapes),
        scratch_shapes=[pltpu.SemaphoreType.DMA((len(shapes),))],
        compiler_params=pltpu.CompilerParams(vmem_limit_bytes=32 << 20),
        cost_estimate=pl.CostEstimate(
            flops=1 << 32, bytes_accessed=2 * count * tokens * (width + LANES) * 2, transcendentals=0
        ),
        name="gather_pages",
    )(table, *caches)
    return [(outs[2 * k], outs[2 * k + 1]) for k in range(len(GROUPS))]


def attention_kernel(offsets, run_len, count, table_ref, q_ref, keys_ref, rotary_ref, out_ref):
    tokens, width = keys_ref.shape[1:]
    packed = q_ref.shape[1] - STAT_ROWS
    slabs = width // LANES
    heads = packed // slabs
    half = tokens // 2
    entry = 2 * (run_len + 1)
    lane = lax.broadcasted_iota(jnp.int32, (heads, LANES), 1)
    rope_lane = lax.broadcasted_iota(jnp.int32, (STAT_ROWS, LANES), 1)
    column = lax.broadcasted_iota(jnp.int32, (heads, tokens), 1)
    over_width = (((1,), (1,)), ((), ()))
    each = range(len(offsets))
    scores, lives = [], []
    for g in each:
        query = jnp.concatenate(
            [q_ref[g, c * heads : (c + 1) * heads, :] for c in range(slabs)], axis=1
        )
        rope = q_ref[g, packed:, :]
        zero = jnp.zeros_like(rope)
        query_rope = jnp.concatenate(
            [jnp.where(rope_lane < ROPE, rope, zero), jnp.where(rope_lane >= ROPE, rope, zero)],
            axis=0,
        )
        score = lax.dot_general(query, keys_ref[g], over_width, preferred_element_type=jnp.float32)
        score = score + lax.dot_general(
            query_rope, rotary_ref[g], over_width, preferred_element_type=jnp.float32
        )
        request = request_at(table_ref, offsets[g], count)
        own_live = table_ref[2 + request * entry + run_len]
        partner_live = table_ref[2 + request * entry + 2 * run_len + 1]
        live = column < jnp.where(column < half, own_live, half + partner_live)
        lives.append(live)
        scores.append(jnp.where(live, score * (1.0 / math.sqrt(NOPE + ROPE)), MASKED_SCORE))
    tops = [jnp.max(score, axis=1, keepdims=True) for score in scores]
    probs = [jnp.where(lives[g], jnp.exp(scores[g] - tops[g]), 0.0) for g in each]
    totals = [jnp.sum(prob, axis=1, keepdims=True) for prob in probs]
    for g in each:
        summed = jnp.dot(
            probs[g].astype(jnp.bfloat16), keys_ref[g], preferred_element_type=jnp.float32
        ).astype(jnp.bfloat16)
        for c in range(slabs):
            out_ref[g, c * heads : (c + 1) * heads, :] = summed[:, c * LANES : (c + 1) * LANES]
    for g in each:
        stats = jnp.zeros((heads, LANES), jnp.float32)
        for i, part in enumerate(parts_of(tops[g], 3) + parts_of(totals[g], 2)):
            stats = jnp.where(lane == i, part, stats)
        out_ref[g, packed:, :] = jnp.zeros((STAT_ROWS, LANES), out_ref.dtype)
        out_ref[g, packed:, :heads] = stats.T[:STAT_ROWS].astype(out_ref.dtype)


def attention(offsets, table, queries, pages, run_len, count):
    groups, rows, _ = queries.shape
    tokens, width = pages[0].shape[1:]
    heads = (rows - STAT_ROWS) * LANES // width
    work = groups * tokens
    return pl.pallas_call(
        lambda *refs: attention_kernel(offsets, run_len, count, *refs),
        out_shape=jax.ShapeDtypeStruct((groups, rows, LANES), jnp.bfloat16),
        in_specs=[pl.BlockSpec(memory_space=pltpu.SMEM)] + [VMEM] * 3,
        out_specs=VMEM,
        compiler_params=LIMIT,
        cost_estimate=pl.CostEstimate(
            flops=work * heads * (4 * width + 4 * ROPE),
            bytes_accessed=work * (width + LANES) * 2,
            transcendentals=work * heads,
        ),
        name="attention",
    )(table, queries, *pages)


def merge_blocks(blocks, packed, heads, final):
    rows = [ref[i, packed:, :].astype(jnp.float32) for ref, i in blocks]
    tops = [r[0:1] + r[1:2] + r[2:3] for r in rows]
    totals = [r[3:4] + r[4:5] for r in rows]
    best = tops[0]
    for top in tops[1:]:
        best = jnp.maximum(best, top)
    weights = [jnp.exp(top - best) for top in tops]
    total = sum(w * t for w, t in zip(weights, totals))
    if final:
        weights = [w / total for w in weights]
    padded = weights + [jnp.zeros_like(best)] * (8 - len(weights))
    columns = jnp.concatenate(padded, axis=0).T
    columns = [columns[:heads, k : k + 1] for k in range(len(blocks))]
    slabs = []
    for c in range(packed // heads):
        slab = 0.0
        for column, (ref, i) in zip(columns, blocks):
            slab += column * ref[i, c * heads : (c + 1) * heads, :].astype(jnp.float32)
        slabs.append(slab.astype(jnp.bfloat16))
    if final:
        return slabs, None
    stats = parts_of(best, 3) + parts_of(total, 2)
    stats += [jnp.zeros((STAT_ROWS - len(stats), LANES), jnp.float32)]
    return slabs, jnp.concatenate(stats, axis=0).astype(jnp.bfloat16)


def near_merge_kernel(heads, sources, *refs):
    inputs, outs = refs[: len(sources)], refs[len(sources) :]
    packed = outs[0].shape[1] - STAT_ROWS
    places = ((0, 0), (1, 0), (1, 1), (2, 0), (2, 1))
    for o, (k, i) in zip(FAR, places):
        blocks = [(ref, held.index(o)) for ref, held in zip(inputs, sources) if o in held]
        slabs, stats = merge_blocks(blocks, packed, heads, False)
        for c, slab in enumerate(slabs):
            outs[k][i, c * heads : (c + 1) * heads, :] = slab
        outs[k][i, packed:, :] = stats


def far_merge_kernel(blocks, *refs):
    inputs, out_ref = refs[:-1], refs[-1]
    heads = out_ref.shape[1]
    packed = inputs[0].shape[1] - STAT_ROWS
    slabs, _ = merge_blocks([(inputs[k], i) for k, i in blocks], packed, heads, True)
    for c, slab in enumerate(slabs):
        out_ref[0, :, c * LANES : (c + 1) * LANES] = slab


def local(q_latent, q_rope, cache_latent, cache_rope, page_table, lengths):
    seq_count = lax.axis_size("seq")
    head_count = lax.axis_size("head")
    my_seq = lax.axis_index("seq")
    my_core = lax.axis_index("head")
    pool_pages, page_len, latent_width = cache_latent.shape
    rope_width = cache_rope.shape[1] // page_len
    request_count, page_slots = page_table.shape
    device_count = seq_count * head_count
    run_len = page_slots // device_count
    heads = q_latent.shape[1]
    reached = [(o + d) % seq_count for d, held in GROUPS for o in held]
    assert sorted(reached) == list(range(seq_count)) and head_count == 2

    rope_rows = q_rope.reshape(2, heads // 2, rope_width)
    rope_rows = jnp.concatenate([rope_rows[0], rope_rows[1]], axis=1)
    block_shape = (1, heads * latent_width // LANES + STAT_ROWS, LANES)
    block = pl.pallas_call(
        pack_kernel,
        out_shape=jax.ShapeDtypeStruct(block_shape, jnp.bfloat16),
        in_specs=[VMEM] * 2,
        out_specs=VMEM,
        compiler_params=LIMIT,
        name="pack",
    )(q_latent, rope_rows)

    other = swapped(block)
    pair = joined("pair", [block, other], ((0, 0), (1, 0)))
    six, thirteen = (shift_from(pair, o) for o in FAR[1:3])

    lat_sent, rope_sent, _ = lax.optimization_barrier((cache_latent, cache_rope, pair))
    partner_lat, partner_rope = swapped(lat_sent), swapped(rope_sent)
    own_rope, partner_rope, table_read = lax.optimization_barrier(
        (cache_rope, partner_rope, page_table)
    )

    def twice(rope):
        rows = rope.reshape(pool_pages, page_len, rope_width)
        return jnp.concatenate([rows, rows], axis=2)

    caches = (cache_latent, partner_lat, twice(own_rope), twice(partner_rope))

    run_owner = table_read[:, ::run_len] // pool_pages
    run_ids = jnp.arange(device_count, dtype=jnp.int32)
    slots = table_read.reshape(request_count, device_count, run_len)

    def runs_on(device):
        here = run_owner == device
        run_index = jnp.sum(jnp.where(here, run_ids[None, :], 0), axis=1)
        pages = jnp.sum(jnp.where(here[:, :, None], slots, 0), axis=1) - device * pool_pages
        live = jnp.clip(lengths - run_index * run_len * page_len, 0, run_len * page_len)
        return [pages, live[:, None]]

    entries = runs_on(my_seq * head_count + my_core)
    entries += runs_on(my_seq * head_count + head_count - 1 - my_core)
    table = jnp.concatenate(entries, axis=1).astype(jnp.int32).reshape(-1)
    place = jnp.stack([my_seq, 1 - 2 * my_core]).astype(jnp.int32)
    table = jnp.concatenate([place, table])
    pages = gather_pages(table, caches, run_len, seq_count)

    six, thirteen, _ = lax.optimization_barrier((six, thirteen, pages[-1][1]))
    crossing = swapped(joined("crossing", [six, thirteen], ((0, 1), (1, 1))))
    where = {0: (0, 0), 6: (1, 0), 13: (2, 0), -6: (3, 0), -13: (3, 1)}
    lists = [held for held in dict.fromkeys(held for _, held in GROUPS)]
    fars = joined(
        "far", [block, six, thirteen, crossing], *[[where[o] for o in held] for held in lists]
    )
    fars = dict(zip(lists, fars))

    near = {d: shift_from(fars[held], d) for d, held in NEAR.items()}
    partials, sources = [], []
    for (d, held), group_pages in zip(GROUPS, pages):
        offsets = tuple(o + d for o in held)
        queries = near[d] if d else fars[held]
        partial = attention(offsets, table, queries, group_pages, run_len, seq_count)
        partials.append(shift_from(partial, -d) if d else partial)
        sources.append(held)

    home, ahead, across = pl.pallas_call(
        lambda *refs: near_merge_kernel(heads, sources, *refs),
        out_shape=[jax.ShapeDtypeStruct((n,) + block_shape[1:], jnp.bfloat16) for n in (1, 2, 2)],
        in_specs=[VMEM] * len(sources),
        out_specs=[VMEM] * 3,
        compiler_params=LIMIT,
        name="near_merge",
    )(*partials)
    taken = swapped(across)
    pair_six, pair_thirteen = joined(
        "pairs", [ahead, taken], ((0, 0), (1, 0)), ((0, 1), (1, 1))
    )
    six, thirteen = shift_from(pair_six, -6), shift_from(pair_thirteen, -13)
    crossing = swapped(joined("crossing_back", [six, thirteen], ((0, 1), (1, 1))))
    arrived = [home, six, thirteen, crossing]
    blocks = ((0, 0), (1, 0), (2, 0), (3, 0), (3, 1))
    return pl.pallas_call(
        lambda *refs: far_merge_kernel(blocks, *refs),
        out_shape=jax.ShapeDtypeStruct((1, heads, latent_width), jnp.bfloat16),
        in_specs=[VMEM] * len(arrived),
        out_specs=VMEM,
        compiler_params=LIMIT,
        name="far_merge",
    )(*arrived)


def solution(mesh):
    return jax.shard_map(
        local,
        mesh=mesh,
        in_specs=(
            P(("groups", "seq"), "head", None),
            P(("groups", "seq"), "head"),
            P(("groups", "seq", "head"), None, None),
            P(("groups", "seq", "head"), None),
            P("groups", None),
            P("groups"),
        ),
        out_specs=P(("groups", "seq"), "head", None),
        check_vma=False,
    )
```

```python
import math

import jax
import jax.numpy as jnp
from jax import lax
from jax.experimental import pallas as pl
from jax.experimental.pallas import tpu as pltpu
from jax.sharding import PartitionSpec as P


ROPE = 64
NOPE = 128
LANES = 128
STAT_ROWS = 16
MASKED_SCORE = -1e30

FAR = (0, 6, 13, -6, -13)
NEAR = {
    1: FAR,
    -1: FAR,
    2: FAR,
    -2: FAR,
    3: (0, 6, 13, -13),
    -3: (0, 13, -6),
}
GROUPS = ((0, FAR),) + tuple(NEAR.items())

VMEM = pl.BlockSpec(memory_space=pltpu.VMEM)
HBM = pl.BlockSpec(memory_space=pltpu.HBM)
LIMIT = pltpu.CompilerParams(vmem_limit_bytes=12 << 20)


def shift_from(array, offset):
    count, cores = lax.axis_size("seq"), lax.axis_size("head")
    pairs = [
        (((i + (1 - 2 * c) * offset) % count) * cores + c, i * cores + c)
        for i in range(count)
        for c in range(cores)
    ]
    return lax.ppermute(array, ("seq", "head"), pairs)


def swapped(array):
    cores = lax.axis_size("head")
    return lax.ppermute(array, "head", [(c, cores - 1 - c) for c in range(cores)])


def joined(arrays, *picks):
    def kernel(*refs):
        for out_ref, pick in zip(refs[len(arrays) :], picks):
            for at, (k, i) in enumerate(pick):
                out_ref[at] = refs[k][i]

    shape = arrays[0].shape[1:]
    outs = pl.pallas_call(
        kernel,
        out_shape=[jax.ShapeDtypeStruct((len(p),) + shape, arrays[0].dtype) for p in picks],
        in_specs=[VMEM] * len(arrays),
        out_specs=[VMEM] * len(picks),
        compiler_params=LIMIT,
    )(*arrays)
    return outs[0] if len(picks) == 1 else outs


def parts_of(x, count):
    parts = []
    for _ in range(count - 1):
        high = x.astype(jnp.bfloat16).astype(jnp.float32)
        parts.append(high)
        x = x - high
    return parts + [x]


def pack_kernel(q_ref, rope_ref, out_ref):
    heads, width = q_ref.shape[1:]
    for c in range(width // LANES):
        out_ref[0, c * heads : (c + 1) * heads, :] = q_ref[0, :, c * LANES : (c + 1) * LANES]
    out_ref[0, heads * width // LANES :, :] = rope_ref[...]


def request_at(table_ref, offset, count):
    return lax.rem(table_ref[0] + table_ref[1] * offset + count, count)


def gather_kernel(run_len, count, table_ref, own_lat, partner_lat, own_rot, partner_rot, *refs):
    outs, sems = refs[:-1], refs[-1]
    entry = 2 * (run_len + 1)
    for k, (d, held) in enumerate(GROUPS):
        keys_ref, rotary_ref = outs[2 * k], outs[2 * k + 1]
        for g, o in enumerate(held):
            request = request_at(table_ref, o + d, count)
            for which, (lat, rot) in enumerate(((own_lat, own_rot), (partner_lat, partner_rot))):
                for j in range(run_len):
                    page = table_ref[2 + request * entry + which * (run_len + 1) + j]
                    slot = which * run_len + j
                    for kind, (cache, to_ref) in enumerate(((lat, keys_ref), (rot, rotary_ref))):
                        size = cache.shape[1]
                        pltpu.make_async_copy(
                            cache.at[page], to_ref.at[g, pl.ds(slot * size, size)], sems.at[2 * k + kind]
                        ).start()
    for k, ref in enumerate(outs):
        pltpu.make_async_copy(ref, ref, sems.at[k]).wait()


def gather_pages(table, caches, run_len, count):
    shapes = []
    for _, held in GROUPS:
        for cache in caches[::2]:
            size, lanes = cache.shape[1:]
            shapes.append(jax.ShapeDtypeStruct((len(held), 2 * run_len * size, lanes), jnp.bfloat16))
    outs = pl.pallas_call(
        lambda *refs: gather_kernel(run_len, count, *refs),
        out_shape=shapes,
        in_specs=[pl.BlockSpec(memory_space=pltpu.SMEM)] + [HBM] * 4,
        out_specs=[VMEM] * len(shapes),
        scratch_shapes=[pltpu.SemaphoreType.DMA((len(shapes),))],
        compiler_params=pltpu.CompilerParams(vmem_limit_bytes=34 << 20),
        cost_estimate=pl.CostEstimate(
            flops=1 << 32, bytes_accessed=2 * sum(s.size * 2 for s in shapes), transcendentals=0
        ),
        name="gather_pages",
    )(table, *caches)
    return [(outs[2 * k], outs[2 * k + 1]) for k in range(len(GROUPS))]


def attention_kernel(offsets, run_len, count, table_ref, q_ref, keys_ref, rotary_ref, out_ref):
    tokens, width = keys_ref.shape[1:]
    packed = q_ref.shape[1] - STAT_ROWS
    slabs = width // LANES
    heads = packed // slabs
    half = tokens // 2
    entry = 2 * (run_len + 1)
    lane = lax.broadcasted_iota(jnp.int32, (heads, LANES), 1)
    rope_lane = lax.broadcasted_iota(jnp.int32, (STAT_ROWS, LANES), 1)
    column = lax.broadcasted_iota(jnp.int32, (heads, tokens), 1)
    row_of = lax.broadcasted_iota(jnp.int32, (tokens, tokens // 2), 0) // 2
    row_in = lax.broadcasted_iota(jnp.int32, (tokens, tokens // 2), 1)
    spread = jnp.where(row_of == row_in, 1.0, 0.0).astype(jnp.bfloat16)
    token_odd = lax.broadcasted_iota(jnp.int32, (tokens, LANES), 0) % 2
    half_of = lax.broadcasted_iota(jnp.int32, (tokens, LANES), 1) // ROPE
    kept = token_odd == half_of
    over_width = (((1,), (1,)), ((), ()))
    each = range(len(offsets))
    scores, lives = [], []
    for g in each:
        query = jnp.concatenate(
            [q_ref[g, c * heads : (c + 1) * heads, :] for c in range(slabs)], axis=1
        )
        rope = q_ref[g, packed:, :].astype(jnp.float32)
        other = pltpu.roll(rope, ROPE, 1)
        query_rope = jnp.concatenate(
            [jnp.where(rope_lane < ROPE, rope, other), jnp.where(rope_lane < ROPE, other, rope)],
            axis=0,
        ).astype(jnp.bfloat16)
        rotary = jnp.dot(spread, rotary_ref[g], preferred_element_type=jnp.float32)
        rotary = jnp.where(kept, rotary, 0.0).astype(jnp.bfloat16)
        score = lax.dot_general(query, keys_ref[g], over_width, preferred_element_type=jnp.float32)
        score = score + lax.dot_general(
            query_rope, rotary, over_width, preferred_element_type=jnp.float32
        )
        request = request_at(table_ref, offsets[g], count)
        own_live = table_ref[2 + request * entry + run_len]
        partner_live = table_ref[2 + request * entry + 2 * run_len + 1]
        live = column < jnp.where(column < half, own_live, half + partner_live)
        lives.append(live)
        scores.append(jnp.where(live, score * (1.0 / math.sqrt(NOPE + ROPE)), MASKED_SCORE))
    tops = [jnp.max(score, axis=1, keepdims=True) for score in scores]
    probs = [jnp.where(lives[g], jnp.exp(scores[g] - tops[g]), 0.0) for g in each]
    totals = [jnp.sum(prob, axis=1, keepdims=True) for prob in probs]
    for g in each:
        summed = jnp.dot(
            probs[g].astype(jnp.bfloat16), keys_ref[g], preferred_element_type=jnp.float32
        ).astype(jnp.bfloat16)
        for c in range(slabs):
            out_ref[g, c * heads : (c + 1) * heads, :] = summed[:, c * LANES : (c + 1) * LANES]
    for g in each:
        stats = jnp.zeros((heads, LANES), jnp.float32)
        for i, part in enumerate(parts_of(tops[g], 3) + parts_of(totals[g], 2)):
            stats = jnp.where(lane == i, part, stats)
        out_ref[g, packed:, :] = jnp.zeros((STAT_ROWS, LANES), out_ref.dtype)
        out_ref[g, packed:, :heads] = stats.T[:STAT_ROWS].astype(out_ref.dtype)


def attention(offsets, table, queries, pages, run_len, count):
    groups, rows, _ = queries.shape
    tokens, width = pages[0].shape[1:]
    heads = (rows - STAT_ROWS) * LANES // width
    work = groups * tokens
    return pl.pallas_call(
        lambda *refs: attention_kernel(offsets, run_len, count, *refs),
        out_shape=jax.ShapeDtypeStruct((groups, rows, LANES), jnp.bfloat16),
        in_specs=[pl.BlockSpec(memory_space=pltpu.SMEM)] + [VMEM] * 3,
        out_specs=VMEM,
        compiler_params=LIMIT,
        cost_estimate=pl.CostEstimate(
            flops=work * heads * (4 * width + 4 * ROPE),
            bytes_accessed=work * (width + LANES) * 2,
            transcendentals=work * heads,
        ),
        name="attention",
    )(table, queries, *pages)


def merge_blocks(blocks, packed, heads, final):
    rows = [ref[i, packed:, :].astype(jnp.float32) for ref, i in blocks]
    tops = [r[0:1] + r[1:2] + r[2:3] for r in rows]
    totals = [r[3:4] + r[4:5] for r in rows]
    best = tops[0]
    for top in tops[1:]:
        best = jnp.maximum(best, top)
    weights = [jnp.exp(top - best) for top in tops]
    total = sum(w * t for w, t in zip(weights, totals))
    if final:
        weights = [w / total for w in weights]
    padded = weights + [jnp.zeros_like(best)] * (8 - len(weights))
    columns = jnp.concatenate(padded, axis=0).T
    columns = [columns[:heads, k : k + 1] for k in range(len(blocks))]
    slabs = []
    for c in range(packed // heads):
        slab = 0.0
        for column, (ref, i) in zip(columns, blocks):
            slab += column * ref[i, c * heads : (c + 1) * heads, :].astype(jnp.float32)
        slabs.append(slab.astype(jnp.bfloat16))
    if final:
        return slabs, None
    stats = parts_of(best, 3) + parts_of(total, 2)
    stats += [jnp.zeros((STAT_ROWS - len(stats), LANES), jnp.float32)]
    return slabs, jnp.concatenate(stats, axis=0).astype(jnp.bfloat16)


def near_merge_kernel(heads, sources, *refs):
    inputs, outs = refs[: len(sources)], refs[len(sources) :]
    packed = outs[0].shape[1] - STAT_ROWS
    places = ((0, 0), (1, 0), (1, 1), (2, 0), (2, 1))
    for o, (k, i) in zip(FAR, places):
        blocks = [(ref, held.index(o)) for ref, held in zip(inputs, sources) if o in held]
        slabs, stats = merge_blocks(blocks, packed, heads, False)
        for c, slab in enumerate(slabs):
            outs[k][i, c * heads : (c + 1) * heads, :] = slab
        outs[k][i, packed:, :] = stats


def far_merge_kernel(blocks, *refs):
    inputs, out_ref = refs[:-1], refs[-1]
    heads = out_ref.shape[1]
    packed = inputs[0].shape[1] - STAT_ROWS
    slabs, _ = merge_blocks([(inputs[k], i) for k, i in blocks], packed, heads, True)
    for c, slab in enumerate(slabs):
        out_ref[0, :, c * LANES : (c + 1) * LANES] = slab


def local(q_latent, q_rope, cache_latent, cache_rope, page_table, lengths):
    seq_count = lax.axis_size("seq")
    head_count = lax.axis_size("head")
    my_seq = lax.axis_index("seq")
    my_core = lax.axis_index("head")
    pool_pages, page_len, latent_width = cache_latent.shape
    rope_width = cache_rope.shape[1] // page_len
    request_count, page_slots = page_table.shape
    device_count = seq_count * head_count
    run_len = page_slots // device_count
    heads = q_latent.shape[1]
    reached = [(o + d) % seq_count for d, held in GROUPS for o in held]
    assert sorted(reached) == list(range(seq_count)) and head_count == 2

    rope_rows = q_rope.reshape(2, heads // 2, rope_width)
    rope_rows = jnp.concatenate([rope_rows[0], rope_rows[1]], axis=1)
    block_shape = (1, heads * latent_width // LANES + STAT_ROWS, LANES)
    block = pl.pallas_call(
        pack_kernel,
        out_shape=jax.ShapeDtypeStruct(block_shape, jnp.bfloat16),
        in_specs=[VMEM] * 2,
        out_specs=VMEM,
        compiler_params=LIMIT,
        name="pack",
    )(q_latent, rope_rows)

    other = swapped(block)
    pair = joined([block, other], ((0, 0), (1, 0)))
    thirteen = shift_from(pair, FAR[2])
    six = shift_from(pair, FAR[1])

    lat_sent, rope_sent, _ = lax.optimization_barrier((cache_latent, cache_rope, pair))
    partner_lat, partner_rope = swapped(lat_sent), swapped(rope_sent)
    own_rope, partner_rope, table_read = lax.optimization_barrier(
        (cache_rope, partner_rope, page_table)
    )

    rows = page_len * rope_width // LANES
    own_rot, partner_rot = (
        rope.reshape(pool_pages, rows, LANES) for rope in (own_rope, partner_rope)
    )
    caches = (cache_latent, partner_lat, own_rot, partner_rot)

    run_owner = table_read[:, ::run_len] // pool_pages
    run_ids = jnp.arange(device_count, dtype=jnp.int32)
    slots = table_read.reshape(request_count, device_count, run_len)

    def runs_on(device):
        here = run_owner == device
        run_index = jnp.sum(jnp.where(here, run_ids[None, :], 0), axis=1)
        pages = jnp.sum(jnp.where(here[:, :, None], slots, 0), axis=1) - device * pool_pages
        live = jnp.clip(lengths - run_index * run_len * page_len, 0, run_len * page_len)
        return [pages, live[:, None]]

    entries = runs_on(my_seq * head_count + my_core)
    entries += runs_on(my_seq * head_count + head_count - 1 - my_core)
    table = jnp.concatenate(entries, axis=1).astype(jnp.int32).reshape(-1)
    place = jnp.stack([my_seq, 1 - 2 * my_core]).astype(jnp.int32)
    table = jnp.concatenate([place, table])
    pages = gather_pages(table, caches, run_len, seq_count)

    six, thirteen, _ = lax.optimization_barrier((six, thirteen, pages[-1][1]))
    crossing = swapped(joined([six, thirteen], ((0, 1), (1, 1))))
    where = {0: (0, 0), 6: (1, 0), 13: (2, 0), -6: (3, 0), -13: (3, 1)}
    lists = [held for held in dict.fromkeys(held for _, held in GROUPS)]
    fars = joined([block, six, thirteen, crossing], *[[where[o] for o in held] for held in lists])
    fars = dict(zip(lists, fars))

    near = {d: shift_from(fars[held], d) for d, held in NEAR.items()}
    partials, sources = [], []
    for (d, held), group_pages in zip(GROUPS, pages):
        offsets = tuple(o + d for o in held)
        queries = near[d] if d else fars[held]
        partial = attention(offsets, table, queries, group_pages, run_len, seq_count)
        partials.append(shift_from(partial, -d) if d else partial)
        sources.append(held)

    home, ahead, across = pl.pallas_call(
        lambda *refs: near_merge_kernel(heads, sources, *refs),
        out_shape=[jax.ShapeDtypeStruct((n,) + block_shape[1:], jnp.bfloat16) for n in (1, 2, 2)],
        in_specs=[VMEM] * len(sources),
        out_specs=[VMEM] * 3,
        compiler_params=LIMIT,
        name="near_merge",
    )(*partials)
    taken = swapped(across)
    pair_six, pair_thirteen = joined([ahead, taken], ((0, 0), (1, 0)), ((0, 1), (1, 1)))
    thirteen = shift_from(pair_thirteen, -FAR[2])
    six = shift_from(pair_six, -FAR[1])
    crossing = swapped(joined([six, thirteen], ((0, 1), (1, 1))))
    arrived = [home, six, thirteen, crossing]
    blocks = ((0, 0), (1, 0), (2, 0), (3, 0), (3, 1))
    return pl.pallas_call(
        lambda *refs: far_merge_kernel(blocks, *refs),
        out_shape=jax.ShapeDtypeStruct((1, heads, latent_width), jnp.bfloat16),
        in_specs=[VMEM] * len(arrived),
        out_specs=VMEM,
        compiler_params=LIMIT,
        name="far_merge",
    )(*arrived)


def solution(mesh):
    return jax.shard_map(
        local,
        mesh=mesh,
        in_specs=(
            P(("groups", "seq"), "head", None),
            P(("groups", "seq"), "head"),
            P(("groups", "seq", "head"), None, None),
            P(("groups", "seq", "head"), None),
            P("groups", None),
            P("groups"),
        ),
        out_specs=P(("groups", "seq"), "head", None),
        check_vma=False,
    )
```

```python
import math

import jax
import jax.numpy as jnp
from jax import lax
from jax.experimental import pallas as pl
from jax.experimental.pallas import tpu as pltpu
from jax.sharding import PartitionSpec as P


ROPE = 64
NOPE = 128
LANES = 128
ROPE_ROWS = 16
STAT_ROWS = 8
MASKED_SCORE = -1e30

FAR = (0, 6, 13, -6, -13)
NEAR = {
    2: FAR,
    -2: FAR,
    1: FAR,
    -1: FAR,
    3: (0, 6, 13, -13),
    -3: (0, 13, -6),
}
GROUPS = ((0, FAR),) + tuple(NEAR.items())

VMEM = pl.BlockSpec(memory_space=pltpu.VMEM)
HBM = pl.BlockSpec(memory_space=pltpu.HBM)
LIMIT = pltpu.CompilerParams(vmem_limit_bytes=12 << 20)


def shift_from(array, offset):
    count, cores = lax.axis_size("seq"), lax.axis_size("head")
    pairs = [
        (((i + (1 - 2 * c) * offset) % count) * cores + c, i * cores + c)
        for i in range(count)
        for c in range(cores)
    ]
    return lax.ppermute(array, ("seq", "head"), pairs)


def swapped(array):
    cores = lax.axis_size("head")
    return lax.ppermute(array, "head", [(c, cores - 1 - c) for c in range(cores)])


def joined(arrays, *picks):
    def kernel(*refs):
        for out_ref, pick in zip(refs[len(arrays) :], picks):
            for at, (k, i) in enumerate(pick):
                out_ref[at] = refs[k][i]

    shape = arrays[0].shape[1:]
    outs = pl.pallas_call(
        kernel,
        out_shape=[jax.ShapeDtypeStruct((len(p),) + shape, arrays[0].dtype) for p in picks],
        in_specs=[VMEM] * len(arrays),
        out_specs=[VMEM] * len(picks),
        compiler_params=LIMIT,
    )(*arrays)
    return outs[0] if len(picks) == 1 else outs


def parts_of(x, count):
    parts = []
    for _ in range(count - 1):
        high = x.astype(jnp.bfloat16).astype(jnp.float32)
        parts.append(high)
        x = x - high
    return parts + [x]


def pack_kernel(q_ref, rope_ref, out_ref):
    heads, width = q_ref.shape[1:]
    for c in range(width // LANES):
        out_ref[0, c * heads : (c + 1) * heads, :] = q_ref[0, :, c * LANES : (c + 1) * LANES]
    out_ref[0, heads * width // LANES :, :] = rope_ref[...]


def request_at(table_ref, offset, count):
    return lax.rem(table_ref[0] + table_ref[1] * offset + count, count)


def gather_kernel(run_len, count, table_ref, own_lat, partner_lat, own_rot, partner_rot, *refs):
    outs, sems = refs[:-1], refs[-1]
    entry = 2 * (run_len + 1)
    for k, (d, held) in enumerate(GROUPS):
        keys_ref, rotary_ref = outs[2 * k], outs[2 * k + 1]
        for g, o in enumerate(held):
            request = request_at(table_ref, o + d, count)
            for which, (lat, rot) in enumerate(((own_lat, own_rot), (partner_lat, partner_rot))):
                for j in range(run_len):
                    page = table_ref[2 + request * entry + which * (run_len + 1) + j]
                    slot = which * run_len + j
                    for kind, (cache, to_ref) in enumerate(((lat, keys_ref), (rot, rotary_ref))):
                        size = cache.shape[1]
                        pltpu.make_async_copy(
                            cache.at[page], to_ref.at[g, pl.ds(slot * size, size)], sems.at[2 * k + kind]
                        ).start()
    for k, ref in enumerate(outs):
        pltpu.make_async_copy(ref, ref, sems.at[k]).wait()


def gather_pages(table, caches, run_len, count):
    shapes = []
    for _, held in GROUPS:
        for cache in caches[::2]:
            size, lanes = cache.shape[1:]
            shapes.append(jax.ShapeDtypeStruct((len(held), 2 * run_len * size, lanes), jnp.bfloat16))
    outs = pl.pallas_call(
        lambda *refs: gather_kernel(run_len, count, *refs),
        out_shape=shapes,
        in_specs=[pl.BlockSpec(memory_space=pltpu.SMEM)] + [HBM] * 4,
        out_specs=[VMEM] * len(shapes),
        scratch_shapes=[pltpu.SemaphoreType.DMA((len(shapes),))],
        compiler_params=pltpu.CompilerParams(vmem_limit_bytes=34 << 20),
        cost_estimate=pl.CostEstimate(
            flops=1 << 32, bytes_accessed=2 * sum(s.size * 2 for s in shapes), transcendentals=0
        ),
        name="gather_pages",
    )(table, *caches)
    return [(outs[2 * k], outs[2 * k + 1]) for k in range(len(GROUPS))]


def attention_kernel(offsets, run_len, count, table_ref, q_ref, keys_ref, rotary_ref, out_ref):
    tokens, width = keys_ref.shape[1:]
    packed = q_ref.shape[1] - ROPE_ROWS
    slabs = width // LANES
    heads = packed // slabs
    half = tokens // 2
    entry = 2 * (run_len + 1)
    lane = lax.broadcasted_iota(jnp.int32, (heads, LANES), 1)
    rope_lane = lax.broadcasted_iota(jnp.int32, (ROPE_ROWS, LANES), 1)
    column = lax.broadcasted_iota(jnp.int32, (heads, tokens), 1)
    row_of = lax.broadcasted_iota(jnp.int32, (tokens, tokens // 2), 0) // 2
    row_in = lax.broadcasted_iota(jnp.int32, (tokens, tokens // 2), 1)
    spread = jnp.where(row_of == row_in, 1.0, 0.0).astype(jnp.bfloat16)
    token_odd = lax.broadcasted_iota(jnp.int32, (tokens, LANES), 0) % 2
    half_of = lax.broadcasted_iota(jnp.int32, (tokens, LANES), 1) // ROPE
    kept = token_odd == half_of
    over_width = (((1,), (1,)), ((), ()))
    each = range(len(offsets))
    scores, lives = [], []
    for g in each:
        query = jnp.concatenate(
            [q_ref[g, c * heads : (c + 1) * heads, :] for c in range(slabs)], axis=1
        )
        rope = q_ref[g, packed:, :].astype(jnp.float32)
        other = pltpu.roll(rope, ROPE, 1)
        query_rope = jnp.concatenate(
            [jnp.where(rope_lane < ROPE, rope, other), jnp.where(rope_lane < ROPE, other, rope)],
            axis=0,
        ).astype(jnp.bfloat16)
        rotary = jnp.dot(spread, rotary_ref[g], preferred_element_type=jnp.float32)
        rotary = jnp.where(kept, rotary, 0.0).astype(jnp.bfloat16)
        score = lax.dot_general(query, keys_ref[g], over_width, preferred_element_type=jnp.float32)
        score = score + lax.dot_general(
            query_rope, rotary, over_width, preferred_element_type=jnp.float32
        )
        request = request_at(table_ref, offsets[g], count)
        own_live = table_ref[2 + request * entry + run_len]
        partner_live = table_ref[2 + request * entry + 2 * run_len + 1]
        live = column < jnp.where(column < half, own_live, half + partner_live)
        lives.append(live)
        scores.append(jnp.where(live, score * (1.0 / math.sqrt(NOPE + ROPE)), MASKED_SCORE))
    tops = [jnp.max(score, axis=1, keepdims=True) for score in scores]
    probs = [jnp.where(lives[g], jnp.exp(scores[g] - tops[g]), 0.0) for g in each]
    totals = [jnp.sum(prob, axis=1, keepdims=True) for prob in probs]
    for g in each:
        summed = jnp.dot(
            probs[g].astype(jnp.bfloat16), keys_ref[g], preferred_element_type=jnp.float32
        ).astype(jnp.bfloat16)
        for c in range(slabs):
            out_ref[g, c * heads : (c + 1) * heads, :] = summed[:, c * LANES : (c + 1) * LANES]
    for g in each:
        stats = jnp.zeros((heads, LANES), jnp.float32)
        for i, part in enumerate(parts_of(tops[g], 3) + parts_of(totals[g], 2)):
            stats = jnp.where(lane == i, part, stats)
        out_ref[g, packed:, :] = jnp.zeros((STAT_ROWS, LANES), out_ref.dtype)
        out_ref[g, packed:, :heads] = stats.T[:STAT_ROWS].astype(out_ref.dtype)


def attention(offsets, table, queries, pages, run_len, count):
    groups, rows, _ = queries.shape
    tokens, width = pages[0].shape[1:]
    packed = rows - ROPE_ROWS
    heads = packed * LANES // width
    work = groups * tokens
    return pl.pallas_call(
        lambda *refs: attention_kernel(offsets, run_len, count, *refs),
        out_shape=jax.ShapeDtypeStruct((groups, packed + STAT_ROWS, LANES), jnp.bfloat16),
        in_specs=[pl.BlockSpec(memory_space=pltpu.SMEM)] + [VMEM] * 3,
        out_specs=VMEM,
        compiler_params=LIMIT,
        cost_estimate=pl.CostEstimate(
            flops=work * heads * (4 * width + 4 * ROPE),
            bytes_accessed=work * (width + LANES) * 2,
            transcendentals=work * heads,
        ),
        name="attention",
    )(table, queries, *pages)


def merge_blocks(blocks, packed, heads, final):
    rows = [ref[i, packed:, :].astype(jnp.float32) for ref, i in blocks]
    tops = [r[0:1] + r[1:2] + r[2:3] for r in rows]
    totals = [r[3:4] + r[4:5] for r in rows]
    best = tops[0]
    for top in tops[1:]:
        best = jnp.maximum(best, top)
    weights = [jnp.exp(top - best) for top in tops]
    total = sum(w * t for w, t in zip(weights, totals))
    if final:
        weights = [w / total for w in weights]
    padded = weights + [jnp.zeros_like(best)] * (8 - len(weights))
    columns = jnp.concatenate(padded, axis=0).T
    columns = [columns[:heads, k : k + 1] for k in range(len(blocks))]
    slabs = []
    for c in range(packed // heads):
        slab = 0.0
        for column, (ref, i) in zip(columns, blocks):
            slab += column * ref[i, c * heads : (c + 1) * heads, :].astype(jnp.float32)
        slabs.append(slab.astype(jnp.bfloat16))
    if final:
        return slabs, None
    stats = parts_of(best, 3) + parts_of(total, 2)
    stats += [jnp.zeros((STAT_ROWS - len(stats), LANES), jnp.float32)]
    return slabs, jnp.concatenate(stats, axis=0).astype(jnp.bfloat16)


def near_merge_kernel(heads, sources, *refs):
    inputs, outs = refs[: len(sources)], refs[len(sources) :]
    packed = outs[0].shape[1] - STAT_ROWS
    places = ((0, 0), (1, 0), (1, 1), (2, 0), (2, 1))
    for o, (k, i) in zip(FAR, places):
        blocks = [(ref, held.index(o)) for ref, held in zip(inputs, sources) if o in held]
        slabs, stats = merge_blocks(blocks, packed, heads, False)
        for c, slab in enumerate(slabs):
            outs[k][i, c * heads : (c + 1) * heads, :] = slab
        outs[k][i, packed:, :] = stats


def far_merge_kernel(blocks, *refs):
    inputs, out_ref = refs[:-1], refs[-1]
    heads = out_ref.shape[1]
    packed = inputs[0].shape[1] - STAT_ROWS
    slabs, _ = merge_blocks([(inputs[k], i) for k, i in blocks], packed, heads, True)
    for c, slab in enumerate(slabs):
        out_ref[0, :, c * LANES : (c + 1) * LANES] = slab


def local(q_latent, q_rope, cache_latent, cache_rope, page_table, lengths):
    seq_count = lax.axis_size("seq")
    head_count = lax.axis_size("head")
    my_seq = lax.axis_index("seq")
    my_core = lax.axis_index("head")
    pool_pages, page_len, latent_width = cache_latent.shape
    rope_width = cache_rope.shape[1] // page_len
    request_count, page_slots = page_table.shape
    device_count = seq_count * head_count
    run_len = page_slots // device_count
    heads = q_latent.shape[1]
    reached = [(o + d) % seq_count for d, held in GROUPS for o in held]
    assert sorted(reached) == list(range(seq_count)) and head_count == 2

    rope_rows = q_rope.reshape(2, heads // 2, rope_width)
    rope_rows = jnp.concatenate([rope_rows[0], rope_rows[1]], axis=1)
    packed = heads * latent_width // LANES
    block_shape = (1, packed + ROPE_ROWS, LANES)
    block = pl.pallas_call(
        pack_kernel,
        out_shape=jax.ShapeDtypeStruct(block_shape, jnp.bfloat16),
        in_specs=[VMEM] * 2,
        out_specs=VMEM,
        compiler_params=LIMIT,
        name="pack",
    )(q_latent, rope_rows)

    other = swapped(block)
    pair = joined([block, other], ((0, 0), (1, 0)))
    thirteen = shift_from(pair, FAR[2])
    six = shift_from(pair, FAR[1])

    lat_sent, rope_sent, _ = lax.optimization_barrier((cache_latent, cache_rope, pair))
    partner_lat, partner_rope = swapped(lat_sent), swapped(rope_sent)
    own_rope, partner_rope, table_read = lax.optimization_barrier(
        (cache_rope, partner_rope, page_table)
    )

    rows = page_len * rope_width // LANES
    own_rot, partner_rot = (
        rope.reshape(pool_pages, rows, LANES) for rope in (own_rope, partner_rope)
    )
    caches = (cache_latent, partner_lat, own_rot, partner_rot)

    run_owner = table_read[:, ::run_len] // pool_pages
    run_ids = jnp.arange(device_count, dtype=jnp.int32)
    slots = table_read.reshape(request_count, device_count, run_len)

    def runs_on(device):
        here = run_owner == device
        run_index = jnp.sum(jnp.where(here, run_ids[None, :], 0), axis=1)
        pages = jnp.sum(jnp.where(here[:, :, None], slots, 0), axis=1) - device * pool_pages
        live = jnp.clip(lengths - run_index * run_len * page_len, 0, run_len * page_len)
        return [pages, live[:, None]]

    entries = runs_on(my_seq * head_count + my_core)
    entries += runs_on(my_seq * head_count + head_count - 1 - my_core)
    table = jnp.concatenate(entries, axis=1).astype(jnp.int32).reshape(-1)
    place = jnp.stack([my_seq, 1 - 2 * my_core]).astype(jnp.int32)
    table = jnp.concatenate([place, table])
    pages = gather_pages(table, caches, run_len, seq_count)

    six, thirteen, _ = lax.optimization_barrier((six, thirteen, pages[-1][1]))
    crossing = swapped(joined([six, thirteen], ((0, 1), (1, 1))))
    where = {0: (0, 0), 6: (1, 0), 13: (2, 0), -6: (3, 0), -13: (3, 1)}
    far = joined([block, six, thirteen, crossing], [where[o] for o in FAR])

    near = {d: shift_from(far, d) for d in (2, -2, 1, -1)}
    for d in (3, -3):
        step = d // 3
        onward = joined([near[2 * step]], [(0, FAR.index(o)) for o in NEAR[d]])
        near[d] = shift_from(onward, step)
    partials, sources = [], []
    for (d, held), group_pages in zip(GROUPS, pages):
        offsets = tuple(o + d for o in held)
        queries = near[d] if d else far
        partial = attention(offsets, table, queries, group_pages, run_len, seq_count)
        partials.append(shift_from(partial, -d) if d else partial)
        sources.append(held)

    home, ahead, across = pl.pallas_call(
        lambda *refs: near_merge_kernel(heads, sources, *refs),
        out_shape=[jax.ShapeDtypeStruct((n, packed + STAT_ROWS, LANES), jnp.bfloat16) for n in (1, 2, 2)],
        in_specs=[VMEM] * len(sources),
        out_specs=[VMEM] * 3,
        compiler_params=LIMIT,
        name="near_merge",
    )(*partials)
    taken = swapped(across)
    pair_six, pair_thirteen = joined([ahead, taken], ((0, 0), (1, 0)), ((0, 1), (1, 1)))
    thirteen = shift_from(pair_thirteen, -FAR[2])
    six = shift_from(pair_six, -FAR[1])
    crossing = swapped(joined([six, thirteen], ((0, 1), (1, 1))))
    arrived = [home, six, thirteen, crossing]
    blocks = ((0, 0), (1, 0), (2, 0), (3, 0), (3, 1))
    return pl.pallas_call(
        lambda *refs: far_merge_kernel(blocks, *refs),
        out_shape=jax.ShapeDtypeStruct((1, heads, latent_width), jnp.bfloat16),
        in_specs=[VMEM] * len(arrived),
        out_specs=VMEM,
        compiler_params=LIMIT,
        name="far_merge",
    )(*arrived)


def solution(mesh):
    return jax.shard_map(
        local,
        mesh=mesh,
        in_specs=(
            P(("groups", "seq"), "head", None),
            P(("groups", "seq"), "head"),
            P(("groups", "seq", "head"), None, None),
            P(("groups", "seq", "head"), None),
            P("groups", None),
            P("groups"),
        ),
        out_specs=P(("groups", "seq"), "head", None),
        check_vma=False,
    )
```

```python
import math

import jax
import jax.numpy as jnp
from jax import lax
from jax.experimental import pallas as pl
from jax.experimental.pallas import tpu as pltpu
from jax.sharding import PartitionSpec as P


ROPE = 64
NOPE = 128
LANES = 128
ROPE_ROWS = 16
STAT_ROWS = 8
MASKED_SCORE = -1e30

FAR = (0, 6, 13, -6, -13)
NEAR = {
    2: FAR,
    -2: FAR,
    1: FAR,
    -1: FAR,
    3: (0, 6, 13, -13),
    -3: (0, 13, -6),
}
GROUPS = ((0, FAR),) + tuple(NEAR.items())

VMEM = pl.BlockSpec(memory_space=pltpu.VMEM)
HBM = pl.BlockSpec(memory_space=pltpu.HBM)
LIMIT = pltpu.CompilerParams(vmem_limit_bytes=12 << 20)


def shift_from(array, offset):
    count, cores = lax.axis_size("seq"), lax.axis_size("head")
    pairs = [
        (((i + (1 - 2 * c) * offset) % count) * cores + c, i * cores + c)
        for i in range(count)
        for c in range(cores)
    ]
    return lax.ppermute(array, ("seq", "head"), pairs)


def swapped(array):
    cores = lax.axis_size("head")
    return lax.ppermute(array, "head", [(c, cores - 1 - c) for c in range(cores)])


def joined(arrays, *picks):
    def kernel(*refs):
        for out_ref, pick in zip(refs[len(arrays) :], picks):
            for at, (k, i) in enumerate(pick):
                out_ref[at] = refs[k][i]

    shape = arrays[0].shape[1:]
    outs = pl.pallas_call(
        kernel,
        out_shape=[jax.ShapeDtypeStruct((len(p),) + shape, arrays[0].dtype) for p in picks],
        in_specs=[VMEM] * len(arrays),
        out_specs=[VMEM] * len(picks),
        compiler_params=LIMIT,
    )(*arrays)
    return outs[0] if len(picks) == 1 else outs


def parts_of(x, count):
    parts = []
    for _ in range(count - 1):
        high = x.astype(jnp.bfloat16).astype(jnp.float32)
        parts.append(high)
        x = x - high
    return parts + [x]


def pack_kernel(q_ref, rope_ref, out_ref):
    heads, width = q_ref.shape[1:]
    for c in range(width // LANES):
        out_ref[0, c * heads : (c + 1) * heads, :] = q_ref[0, :, c * LANES : (c + 1) * LANES]
    out_ref[0, heads * width // LANES :, :] = rope_ref[...]


def request_at(table_ref, offset, count):
    return lax.rem(table_ref[0] + table_ref[1] * offset + count, count)


def gather_kernel(run_len, count, table_ref, own_lat, partner_lat, own_rot, partner_rot, *refs):
    n = len(GROUPS)
    keys_refs, rotary_refs, buffers = refs[:n], refs[n : 2 * n], refs[2 * n : 3 * n]
    lat_sems, rot_sems = refs[3 * n :]
    entry = 2 * (run_len + 1)
    for k, (d, held) in enumerate(GROUPS):
        for g, o in enumerate(held):
            request = request_at(table_ref, o + d, count)
            for which, (lat, rot) in enumerate(((own_lat, own_rot), (partner_lat, partner_rot))):
                for j in range(run_len):
                    page = table_ref[2 + request * entry + which * (run_len + 1) + j]
                    slot = which * run_len + j
                    for cache, to_ref, sems in (
                        (rot, buffers[k], rot_sems),
                        (lat, keys_refs[k], lat_sems),
                    ):
                        size = cache.shape[1]
                        pltpu.make_async_copy(
                            cache.at[page], to_ref.at[g, pl.ds(slot * size, size)], sems.at[k]
                        ).start()

    tokens = rotary_refs[0].shape[1]
    row_of = lax.broadcasted_iota(jnp.int32, (tokens, tokens // 2), 0) // 2
    row_in = lax.broadcasted_iota(jnp.int32, (tokens, tokens // 2), 1)
    spread = jnp.where(row_of == row_in, 1.0, 0.0).astype(jnp.bfloat16)
    token_odd = lax.broadcasted_iota(jnp.int32, (tokens, LANES), 0) % 2
    kept = token_odd == lax.broadcasted_iota(jnp.int32, (tokens, LANES), 1) // ROPE
    for k, (ref, buffer) in enumerate(zip(rotary_refs, buffers)):
        pltpu.make_async_copy(buffer, buffer, rot_sems.at[k]).wait()
        for g in range(ref.shape[0]):
            rows = jnp.dot(spread, buffer[g], preferred_element_type=jnp.float32)
            ref[g] = jnp.where(kept, rows, 0.0).astype(ref.dtype)
    for k, ref in enumerate(keys_refs):
        pltpu.make_async_copy(ref, ref, lat_sems.at[k]).wait()


def gather_pages(table, caches, run_len, count):
    page_len, width = caches[0].shape[1:]
    rows = caches[2].shape[1]
    pages = 2 * run_len

    def shapes(size, lanes):
        return [(len(held), pages * size, lanes) for _, held in GROUPS]

    made = shapes(page_len, width) + shapes(page_len, LANES)
    outs = pl.pallas_call(
        lambda *refs: gather_kernel(run_len, count, *refs),
        out_shape=[jax.ShapeDtypeStruct(shape, jnp.bfloat16) for shape in made],
        in_specs=[pl.BlockSpec(memory_space=pltpu.SMEM)] + [HBM] * 4,
        out_specs=[VMEM] * len(made),
        scratch_shapes=[pltpu.VMEM(shape, jnp.bfloat16) for shape in shapes(rows, LANES)]
        + [pltpu.SemaphoreType.DMA((len(GROUPS),))] * 2,
        compiler_params=pltpu.CompilerParams(vmem_limit_bytes=34 << 20),
        cost_estimate=pl.CostEstimate(
            flops=1 << 32,
            bytes_accessed=4 * sum(math.prod(shape) for shape in made),
            transcendentals=0,
        ),
        name="gather_pages",
    )(table, *caches)
    return list(zip(outs[: len(GROUPS)], outs[len(GROUPS) :]))


def attention_kernel(offsets, run_len, count, table_ref, q_ref, keys_ref, rotary_ref, out_ref):
    tokens, width = keys_ref.shape[1:]
    packed = q_ref.shape[1] - ROPE_ROWS
    slabs = width // LANES
    heads = packed // slabs
    half = tokens // 2
    entry = 2 * (run_len + 1)
    lane = lax.broadcasted_iota(jnp.int32, (heads, LANES), 1)
    rope_lane = lax.broadcasted_iota(jnp.int32, (ROPE_ROWS, LANES), 1)
    column = lax.broadcasted_iota(jnp.int32, (heads, tokens), 1)
    over_width = (((1,), (1,)), ((), ()))
    each = range(len(offsets))
    scores, lives = [], []
    for g in each:
        query = jnp.concatenate(
            [q_ref[g, c * heads : (c + 1) * heads, :] for c in range(slabs)], axis=1
        )
        rope = q_ref[g, packed:, :].astype(jnp.float32)
        other = pltpu.roll(rope, ROPE, 1)
        query_rope = jnp.concatenate(
            [jnp.where(rope_lane < ROPE, rope, other), jnp.where(rope_lane < ROPE, other, rope)],
            axis=0,
        ).astype(jnp.bfloat16)
        score = lax.dot_general(query, keys_ref[g], over_width, preferred_element_type=jnp.float32)
        score = score + lax.dot_general(
            query_rope, rotary_ref[g], over_width, preferred_element_type=jnp.float32
        )
        request = request_at(table_ref, offsets[g], count)
        own_live = table_ref[2 + request * entry + run_len]
        partner_live = table_ref[2 + request * entry + 2 * run_len + 1]
        live = column < jnp.where(column < half, own_live, half + partner_live)
        lives.append(live)
        scores.append(jnp.where(live, score * (1.0 / math.sqrt(NOPE + ROPE)), MASKED_SCORE))
    tops = [jnp.max(score, axis=1, keepdims=True) for score in scores]
    probs = [jnp.where(lives[g], jnp.exp(scores[g] - tops[g]), 0.0) for g in each]
    totals = [jnp.sum(prob, axis=1, keepdims=True) for prob in probs]
    for g in each:
        summed = jnp.dot(
            probs[g].astype(jnp.bfloat16), keys_ref[g], preferred_element_type=jnp.float32
        ).astype(jnp.bfloat16)
        for c in range(slabs):
            out_ref[g, c * heads : (c + 1) * heads, :] = summed[:, c * LANES : (c + 1) * LANES]
    for g in each:
        stats = jnp.zeros((heads, LANES), jnp.float32)
        for i, part in enumerate(parts_of(tops[g], 3) + parts_of(totals[g], 2)):
            stats = jnp.where(lane == i, part, stats)
        out_ref[g, packed:, :] = jnp.zeros((STAT_ROWS, LANES), out_ref.dtype)
        out_ref[g, packed:, :heads] = stats.T[:STAT_ROWS].astype(out_ref.dtype)


def attention(offsets, table, queries, pages, run_len, count):
    groups, rows, _ = queries.shape
    tokens, width = pages[0].shape[1:]
    packed = rows - ROPE_ROWS
    heads = packed * LANES // width
    work = groups * tokens
    return pl.pallas_call(
        lambda *refs: attention_kernel(offsets, run_len, count, *refs),
        out_shape=jax.ShapeDtypeStruct((groups, packed + STAT_ROWS, LANES), jnp.bfloat16),
        in_specs=[pl.BlockSpec(memory_space=pltpu.SMEM)] + [VMEM] * 3,
        out_specs=VMEM,
        compiler_params=LIMIT,
        cost_estimate=pl.CostEstimate(
            flops=work * heads * (4 * width + 4 * ROPE),
            bytes_accessed=work * (width + LANES) * 2,
            transcendentals=work * heads,
        ),
        name="attention",
    )(table, queries, *pages)


def merge_blocks(blocks, packed, heads, final):
    rows = [ref[i, packed:, :].astype(jnp.float32) for ref, i in blocks]
    tops = [r[0:1] + r[1:2] + r[2:3] for r in rows]
    totals = [r[3:4] + r[4:5] for r in rows]
    best = tops[0]
    for top in tops[1:]:
        best = jnp.maximum(best, top)
    weights = [jnp.exp(top - best) for top in tops]
    total = sum(w * t for w, t in zip(weights, totals))
    if final:
        weights = [w / total for w in weights]
    padded = weights + [jnp.zeros_like(best)] * (8 - len(weights))
    columns = jnp.concatenate(padded, axis=0).T
    columns = [columns[:heads, k : k + 1] for k in range(len(blocks))]
    slabs = []
    for c in range(packed // heads):
        slab = 0.0
        for column, (ref, i) in zip(columns, blocks):
            slab += column * ref[i, c * heads : (c + 1) * heads, :].astype(jnp.float32)
        slabs.append(slab.astype(jnp.bfloat16))
    if final:
        return slabs, None
    stats = parts_of(best, 3) + parts_of(total, 2)
    stats += [jnp.zeros((STAT_ROWS - len(stats), LANES), jnp.float32)]
    return slabs, jnp.concatenate(stats, axis=0).astype(jnp.bfloat16)


def near_merge_kernel(heads, sources, *refs):
    inputs, outs = refs[: len(sources)], refs[len(sources) :]
    packed = outs[0].shape[1] - STAT_ROWS
    places = ((0, 0), (1, 0), (1, 1), (2, 0), (2, 1))
    for o, (k, i) in zip(FAR, places):
        blocks = [(ref, held.index(o)) for ref, held in zip(inputs, sources) if o in held]
        slabs, stats = merge_blocks(blocks, packed, heads, False)
        for c, slab in enumerate(slabs):
            outs[k][i, c * heads : (c + 1) * heads, :] = slab
        outs[k][i, packed:, :] = stats


def far_merge_kernel(blocks, *refs):
    inputs, out_ref = refs[:-1], refs[-1]
    heads = out_ref.shape[1]
    packed = inputs[0].shape[1] - STAT_ROWS
    slabs, _ = merge_blocks([(inputs[k], i) for k, i in blocks], packed, heads, True)
    for c, slab in enumerate(slabs):
        out_ref[0, :, c * LANES : (c + 1) * LANES] = slab


def local(q_latent, q_rope, cache_latent, cache_rope, page_table, lengths):
    seq_count = lax.axis_size("seq")
    head_count = lax.axis_size("head")
    my_seq = lax.axis_index("seq")
    my_core = lax.axis_index("head")
    pool_pages, page_len, latent_width = cache_latent.shape
    rope_width = cache_rope.shape[1] // page_len
    request_count, page_slots = page_table.shape
    device_count = seq_count * head_count
    run_len = page_slots // device_count
    heads = q_latent.shape[1]
    reached = [(o + d) % seq_count for d, held in GROUPS for o in held]
    assert sorted(reached) == list(range(seq_count)) and head_count == 2

    rope_rows = q_rope.reshape(2, heads // 2, rope_width)
    rope_rows = jnp.concatenate([rope_rows[0], rope_rows[1]], axis=1)
    packed = heads * latent_width // LANES
    block_shape = (1, packed + ROPE_ROWS, LANES)
    block = pl.pallas_call(
        pack_kernel,
        out_shape=jax.ShapeDtypeStruct(block_shape, jnp.bfloat16),
        in_specs=[VMEM] * 2,
        out_specs=VMEM,
        compiler_params=LIMIT,
        name="pack",
    )(q_latent, rope_rows)

    other = swapped(block)
    pair = joined([block, other], ((0, 0), (1, 0)))
    thirteen = shift_from(pair, FAR[2])
    six = shift_from(pair, FAR[1])

    lat_sent, rope_sent, _ = lax.optimization_barrier((cache_latent, cache_rope, pair))
    partner_lat, partner_rope = swapped(lat_sent), swapped(rope_sent)
    own_rope, partner_rope, table_read = lax.optimization_barrier(
        (cache_rope, partner_rope, page_table)
    )

    rows = page_len * rope_width // LANES
    own_rot, partner_rot = (
        rope.reshape(pool_pages, rows, LANES) for rope in (own_rope, partner_rope)
    )
    caches = (cache_latent, partner_lat, own_rot, partner_rot)

    run_owner = table_read[:, ::run_len] // pool_pages
    run_ids = jnp.arange(device_count, dtype=jnp.int32)
    slots = table_read.reshape(request_count, device_count, run_len)

    def runs_on(device):
        here = run_owner == device
        run_index = jnp.sum(jnp.where(here, run_ids[None, :], 0), axis=1)
        pages = jnp.sum(jnp.where(here[:, :, None], slots, 0), axis=1) - device * pool_pages
        live = jnp.clip(lengths - run_index * run_len * page_len, 0, run_len * page_len)
        return [pages, live[:, None]]

    entries = runs_on(my_seq * head_count + my_core)
    entries += runs_on(my_seq * head_count + head_count - 1 - my_core)
    table = jnp.concatenate(entries, axis=1).astype(jnp.int32).reshape(-1)
    place = jnp.stack([my_seq, 1 - 2 * my_core]).astype(jnp.int32)
    table = jnp.concatenate([place, table])
    pages = gather_pages(table, caches, run_len, seq_count)

    six, thirteen, _ = lax.optimization_barrier((six, thirteen, pages[-1][1]))
    crossing = swapped(joined([six, thirteen], ((0, 1), (1, 1))))
    where = {0: (0, 0), 6: (1, 0), 13: (2, 0), -6: (3, 0), -13: (3, 1)}
    lists = [held for held in dict.fromkeys(held for _, held in GROUPS)]
    fars = joined([block, six, thirteen, crossing], *[[where[o] for o in held] for held in lists])
    fars = dict(zip(lists, fars))

    near = {d: shift_from(fars[held], d) for d, held in NEAR.items()}
    partials, sources = [], []
    for (d, held), group_pages in zip(GROUPS, pages):
        offsets = tuple(o + d for o in held)
        queries = near[d] if d else fars[held]
        partial = attention(offsets, table, queries, group_pages, run_len, seq_count)
        partials.append(shift_from(partial, -d) if d else partial)
        sources.append(held)

    home, ahead, across = pl.pallas_call(
        lambda *refs: near_merge_kernel(heads, sources, *refs),
        out_shape=[jax.ShapeDtypeStruct((n, packed + STAT_ROWS, LANES), jnp.bfloat16) for n in (1, 2, 2)],
        in_specs=[VMEM] * len(sources),
        out_specs=[VMEM] * 3,
        compiler_params=LIMIT,
        name="near_merge",
    )(*partials)
    taken = swapped(across)
    pair_six, pair_thirteen = joined([ahead, taken], ((0, 0), (1, 0)), ((0, 1), (1, 1)))
    thirteen = shift_from(pair_thirteen, -FAR[2])
    six = shift_from(pair_six, -FAR[1])
    crossing = swapped(joined([six, thirteen], ((0, 1), (1, 1))))
    arrived = [home, six, thirteen, crossing]
    blocks = ((0, 0), (1, 0), (2, 0), (3, 0), (3, 1))
    return pl.pallas_call(
        lambda *refs: far_merge_kernel(blocks, *refs),
        out_shape=jax.ShapeDtypeStruct((1, heads, latent_width), jnp.bfloat16),
        in_specs=[VMEM] * len(arrived),
        out_specs=VMEM,
        compiler_params=LIMIT,
        name="far_merge",
    )(*arrived)


def solution(mesh):
    return jax.shard_map(
        local,
        mesh=mesh,
        in_specs=(
            P(("groups", "seq"), "head", None),
            P(("groups", "seq"), "head"),
            P(("groups", "seq", "head"), None, None),
            P(("groups", "seq", "head"), None),
            P("groups", None),
            P("groups"),
        ),
        out_specs=P(("groups", "seq"), "head", None),
        check_vma=False,
    )
```

```python
import math

import jax
import jax.numpy as jnp
from jax import lax
from jax.experimental import pallas as pl
from jax.experimental.pallas import tpu as pltpu
from jax.sharding import PartitionSpec as P


ROPE = 64
NOPE = 128
LANES = 128
ROPE_ROWS = 16
STAT_ROWS = 8
MASKED_SCORE = -1e30

FAR = (0, 6, 13, -6, -13)
NEAR = {
    3: (0, 6, 13, -13),
    -3: (0, 13, -6),
    2: FAR,
    -2: FAR,
    1: FAR,
    -1: FAR,
}
GROUPS = ((0, FAR),) + tuple(NEAR.items())

VMEM = pl.BlockSpec(memory_space=pltpu.VMEM)
HBM = pl.BlockSpec(memory_space=pltpu.HBM)
LIMIT = pltpu.CompilerParams(vmem_limit_bytes=12 << 20)


def shift_from(array, offset):
    count, cores = lax.axis_size("seq"), lax.axis_size("head")
    pairs = [
        (((i + (1 - 2 * c) * offset) % count) * cores + c, i * cores + c)
        for i in range(count)
        for c in range(cores)
    ]
    return lax.ppermute(array, ("seq", "head"), pairs)


def swapped(array):
    cores = lax.axis_size("head")
    return lax.ppermute(array, "head", [(c, cores - 1 - c) for c in range(cores)])


def joined(arrays, *picks):
    def kernel(*refs):
        for out_ref, pick in zip(refs[len(arrays) :], picks):
            for at, (k, i) in enumerate(pick):
                out_ref[at] = refs[k][i]

    shape = arrays[0].shape[1:]
    outs = pl.pallas_call(
        kernel,
        out_shape=[jax.ShapeDtypeStruct((len(p),) + shape, arrays[0].dtype) for p in picks],
        in_specs=[VMEM] * len(arrays),
        out_specs=[VMEM] * len(picks),
        compiler_params=LIMIT,
    )(*arrays)
    return outs[0] if len(picks) == 1 else outs


def parts_of(x, count):
    parts = []
    for _ in range(count - 1):
        high = x.astype(jnp.bfloat16).astype(jnp.float32)
        parts.append(high)
        x = x - high
    return parts + [x]


def pack_kernel(q_ref, rope_ref, out_ref):
    heads, width = q_ref.shape[1:]
    for c in range(width // LANES):
        out_ref[0, c * heads : (c + 1) * heads, :] = q_ref[0, :, c * LANES : (c + 1) * LANES]
    out_ref[0, heads * width // LANES :, :] = rope_ref[...]


def request_at(table_ref, offset, count):
    return lax.rem(table_ref[0] + table_ref[1] * offset + count, count)


def gather_kernel(run_len, count, table_ref, own_lat, partner_lat, own_rot, partner_rot, *refs):
    n = len(GROUPS)
    keys_refs, rotary_refs, buffers = refs[:n], refs[n : 2 * n], refs[2 * n : 3 * n]
    lat_sems, rot_sems = refs[3 * n :]
    entry = 2 * (run_len + 1)
    for k, (d, held) in enumerate(GROUPS):
        for g, o in enumerate(held):
            request = request_at(table_ref, o + d, count)
            for which, (lat, rot) in enumerate(((own_lat, own_rot), (partner_lat, partner_rot))):
                for j in range(run_len):
                    page = table_ref[2 + request * entry + which * (run_len + 1) + j]
                    slot = which * run_len + j
                    for cache, to_ref, sems in (
                        (rot, buffers[k], rot_sems),
                        (lat, keys_refs[k], lat_sems),
                    ):
                        size = cache.shape[1]
                        pltpu.make_async_copy(
                            cache.at[page], to_ref.at[g, pl.ds(slot * size, size)], sems.at[k]
                        ).start()

    tokens = rotary_refs[0].shape[1]
    row_of = lax.broadcasted_iota(jnp.int32, (tokens, tokens // 2), 0) // 2
    row_in = lax.broadcasted_iota(jnp.int32, (tokens, tokens // 2), 1)
    spread = jnp.where(row_of == row_in, 1.0, 0.0).astype(jnp.bfloat16)
    token_odd = lax.broadcasted_iota(jnp.int32, (tokens, LANES), 0) % 2
    kept = token_odd == lax.broadcasted_iota(jnp.int32, (tokens, LANES), 1) // ROPE
    for k, (ref, buffer) in enumerate(zip(rotary_refs, buffers)):
        pltpu.make_async_copy(buffer, buffer, rot_sems.at[k]).wait()
        for g in range(ref.shape[0]):
            rows = jnp.dot(spread, buffer[g], preferred_element_type=jnp.float32)
            ref[g] = jnp.where(kept, rows, 0.0).astype(ref.dtype)
    for k, ref in enumerate(keys_refs):
        pltpu.make_async_copy(ref, ref, lat_sems.at[k]).wait()


def gather_pages(table, caches, run_len, count):
    page_len, width = caches[0].shape[1:]
    rows = caches[2].shape[1]
    pages = 2 * run_len

    def shapes(size, lanes):
        return [(len(held), pages * size, lanes) for _, held in GROUPS]

    made = shapes(page_len, width) + shapes(page_len, LANES)
    outs = pl.pallas_call(
        lambda *refs: gather_kernel(run_len, count, *refs),
        out_shape=[jax.ShapeDtypeStruct(shape, jnp.bfloat16) for shape in made],
        in_specs=[pl.BlockSpec(memory_space=pltpu.SMEM)] + [HBM] * 4,
        out_specs=[VMEM] * len(made),
        scratch_shapes=[pltpu.VMEM(shape, jnp.bfloat16) for shape in shapes(rows, LANES)]
        + [pltpu.SemaphoreType.DMA((len(GROUPS),))] * 2,
        compiler_params=pltpu.CompilerParams(vmem_limit_bytes=34 << 20),
        cost_estimate=pl.CostEstimate(
            flops=1 << 32,
            bytes_accessed=4 * sum(math.prod(shape) for shape in made),
            transcendentals=0,
        ),
        name="gather_pages",
    )(table, *caches)
    return list(zip(outs[: len(GROUPS)], outs[len(GROUPS) :]))


def attention_kernel(offsets, run_len, count, table_ref, q_ref, keys_ref, rotary_ref, out_ref):
    tokens, width = keys_ref.shape[1:]
    packed = q_ref.shape[1] - ROPE_ROWS
    slabs = width // LANES
    heads = packed // slabs
    half = tokens // 2
    entry = 2 * (run_len + 1)
    lane = lax.broadcasted_iota(jnp.int32, (heads, LANES), 1)
    rope_lane = lax.broadcasted_iota(jnp.int32, (ROPE_ROWS, LANES), 1)
    column = lax.broadcasted_iota(jnp.int32, (heads, tokens), 1)
    over_width = (((1,), (1,)), ((), ()))
    each = range(len(offsets))
    scores, lives = [], []
    for g in each:
        query = jnp.concatenate(
            [q_ref[g, c * heads : (c + 1) * heads, :] for c in range(slabs)], axis=1
        )
        rope = q_ref[g, packed:, :].astype(jnp.float32)
        other = pltpu.roll(rope, ROPE, 1)
        query_rope = jnp.concatenate(
            [jnp.where(rope_lane < ROPE, rope, other), jnp.where(rope_lane < ROPE, other, rope)],
            axis=0,
        ).astype(jnp.bfloat16)
        score = lax.dot_general(query, keys_ref[g], over_width, preferred_element_type=jnp.float32)
        score = score + lax.dot_general(
            query_rope, rotary_ref[g], over_width, preferred_element_type=jnp.float32
        )
        request = request_at(table_ref, offsets[g], count)
        own_live = table_ref[2 + request * entry + run_len]
        partner_live = table_ref[2 + request * entry + 2 * run_len + 1]
        live = column < jnp.where(column < half, own_live, half + partner_live)
        lives.append(live)
        scores.append(jnp.where(live, score * (1.0 / math.sqrt(NOPE + ROPE)), MASKED_SCORE))
    tops = [jnp.max(score, axis=1, keepdims=True) for score in scores]
    probs = [jnp.where(lives[g], jnp.exp(scores[g] - tops[g]), 0.0) for g in each]
    totals = [jnp.sum(prob, axis=1, keepdims=True) for prob in probs]
    for g in each:
        summed = jnp.dot(
            probs[g].astype(jnp.bfloat16), keys_ref[g], preferred_element_type=jnp.float32
        ).astype(jnp.bfloat16)
        for c in range(slabs):
            out_ref[g, c * heads : (c + 1) * heads, :] = summed[:, c * LANES : (c + 1) * LANES]
    for g in each:
        stats = jnp.zeros((heads, LANES), jnp.float32)
        for i, part in enumerate(parts_of(tops[g], 3) + parts_of(totals[g], 2)):
            stats = jnp.where(lane == i, part, stats)
        out_ref[g, packed:, :] = jnp.zeros((STAT_ROWS, LANES), out_ref.dtype)
        out_ref[g, packed:, :heads] = stats.T[:STAT_ROWS].astype(out_ref.dtype)


def attention(offsets, table, queries, pages, run_len, count):
    groups, rows, _ = queries.shape
    tokens, width = pages[0].shape[1:]
    packed = rows - ROPE_ROWS
    heads = packed * LANES // width
    work = groups * tokens
    return pl.pallas_call(
        lambda *refs: attention_kernel(offsets, run_len, count, *refs),
        out_shape=jax.ShapeDtypeStruct((groups, packed + STAT_ROWS, LANES), jnp.bfloat16),
        in_specs=[pl.BlockSpec(memory_space=pltpu.SMEM)] + [VMEM] * 3,
        out_specs=VMEM,
        compiler_params=LIMIT,
        cost_estimate=pl.CostEstimate(
            flops=work * heads * (4 * width + 4 * ROPE),
            bytes_accessed=work * (width + LANES) * 2,
            transcendentals=work * heads,
        ),
        name="attention",
    )(table, queries, *pages)


def merge_blocks(blocks, packed, heads, final):
    rows = [ref[i, packed:, :].astype(jnp.float32) for ref, i in blocks]
    tops = [r[0:1] + r[1:2] + r[2:3] for r in rows]
    totals = [r[3:4] + r[4:5] for r in rows]
    best = tops[0]
    for top in tops[1:]:
        best = jnp.maximum(best, top)
    weights = [jnp.exp(top - best) for top in tops]
    total = sum(w * t for w, t in zip(weights, totals))
    if final:
        weights = [w / total for w in weights]
    padded = weights + [jnp.zeros_like(best)] * (8 - len(weights))
    columns = jnp.concatenate(padded, axis=0).T
    columns = [columns[:heads, k : k + 1] for k in range(len(blocks))]
    slabs = []
    for c in range(packed // heads):
        slab = 0.0
        for column, (ref, i) in zip(columns, blocks):
            slab += column * ref[i, c * heads : (c + 1) * heads, :].astype(jnp.float32)
        slabs.append(slab.astype(jnp.bfloat16))
    if final:
        return slabs, None
    stats = parts_of(best, 3) + parts_of(total, 2)
    stats += [jnp.zeros((STAT_ROWS - len(stats), LANES), jnp.float32)]
    return slabs, jnp.concatenate(stats, axis=0).astype(jnp.bfloat16)


def near_merge_kernel(heads, sources, *refs):
    inputs, outs = refs[: len(sources)], refs[len(sources) :]
    packed = outs[0].shape[1] - STAT_ROWS
    places = ((0, 0), (1, 0), (1, 1), (2, 0), (2, 1))
    for o, (k, i) in zip(FAR, places):
        blocks = [(ref, held.index(o)) for ref, held in zip(inputs, sources) if o in held]
        slabs, stats = merge_blocks(blocks, packed, heads, False)
        for c, slab in enumerate(slabs):
            outs[k][i, c * heads : (c + 1) * heads, :] = slab
        outs[k][i, packed:, :] = stats


def far_merge_kernel(blocks, *refs):
    inputs, out_ref = refs[:-1], refs[-1]
    heads = out_ref.shape[1]
    packed = inputs[0].shape[1] - STAT_ROWS
    slabs, _ = merge_blocks([(inputs[k], i) for k, i in blocks], packed, heads, True)
    for c, slab in enumerate(slabs):
        out_ref[0, :, c * LANES : (c + 1) * LANES] = slab


def local(q_latent, q_rope, cache_latent, cache_rope, page_table, lengths):
    seq_count = lax.axis_size("seq")
    head_count = lax.axis_size("head")
    my_seq = lax.axis_index("seq")
    my_core = lax.axis_index("head")
    pool_pages, page_len, latent_width = cache_latent.shape
    rope_width = cache_rope.shape[1] // page_len
    request_count, page_slots = page_table.shape
    device_count = seq_count * head_count
    run_len = page_slots // device_count
    heads = q_latent.shape[1]
    reached = [(o + d) % seq_count for d, held in GROUPS for o in held]
    assert sorted(reached) == list(range(seq_count)) and head_count == 2

    rope_rows = q_rope.reshape(2, heads // 2, rope_width)
    rope_rows = jnp.concatenate([rope_rows[0], rope_rows[1]], axis=1)
    packed = heads * latent_width // LANES
    block_shape = (1, packed + ROPE_ROWS, LANES)
    block = pl.pallas_call(
        pack_kernel,
        out_shape=jax.ShapeDtypeStruct(block_shape, jnp.bfloat16),
        in_specs=[VMEM] * 2,
        out_specs=VMEM,
        compiler_params=LIMIT,
        name="pack",
    )(q_latent, rope_rows)

    other = swapped(block)
    pair = joined([block, other], ((0, 0), (1, 0)))
    thirteen = shift_from(pair, FAR[2])
    six = shift_from(pair, FAR[1])

    lat_sent, rope_sent, _ = lax.optimization_barrier((cache_latent, cache_rope, pair))
    partner_lat, partner_rope = swapped(lat_sent), swapped(rope_sent)
    own_rope, partner_rope, table_read = lax.optimization_barrier(
        (cache_rope, partner_rope, page_table)
    )

    rows = page_len * rope_width // LANES
    own_rot, partner_rot = (
        rope.reshape(pool_pages, rows, LANES) for rope in (own_rope, partner_rope)
    )
    caches = (cache_latent, partner_lat, own_rot, partner_rot)

    run_owner = table_read[:, ::run_len] // pool_pages
    run_ids = jnp.arange(device_count, dtype=jnp.int32)
    slots = table_read.reshape(request_count, device_count, run_len)

    def runs_on(device):
        here = run_owner == device
        run_index = jnp.sum(jnp.where(here, run_ids[None, :], 0), axis=1)
        pages = jnp.sum(jnp.where(here[:, :, None], slots, 0), axis=1) - device * pool_pages
        live = jnp.clip(lengths - run_index * run_len * page_len, 0, run_len * page_len)
        return [pages, live[:, None]]

    entries = runs_on(my_seq * head_count + my_core)
    entries += runs_on(my_seq * head_count + head_count - 1 - my_core)
    table = jnp.concatenate(entries, axis=1).astype(jnp.int32).reshape(-1)
    place = jnp.stack([my_seq, 1 - 2 * my_core]).astype(jnp.int32)
    table = jnp.concatenate([place, table])
    pages = gather_pages(table, caches, run_len, seq_count)

    six, thirteen, _ = lax.optimization_barrier((six, thirteen, pages[-1][1]))
    crossing = swapped(joined([six, thirteen], ((0, 1), (1, 1))))
    where = {0: (0, 0), 6: (1, 0), 13: (2, 0), -6: (3, 0), -13: (3, 1)}
    lists = [held for held in dict.fromkeys(held for _, held in GROUPS)]
    fars = joined([block, six, thirteen, crossing], *[[where[o] for o in held] for held in lists])
    fars = dict(zip(lists, fars))

    near = {}
    for d, held in NEAR.items():
        near[d] = shift_from(fars[held], d)
    partials, sources = [], []
    for (d, held), group_pages in zip(GROUPS, pages):
        offsets = tuple(o + d for o in held)
        queries = near[d] if d else fars[held]
        partial = attention(offsets, table, queries, group_pages, run_len, seq_count)
        if d:
            partial = shift_from(partial, -d)
        partials.append(partial)
        sources.append(held)

    home, ahead, across = pl.pallas_call(
        lambda *refs: near_merge_kernel(heads, sources, *refs),
        out_shape=[jax.ShapeDtypeStruct((n, packed + STAT_ROWS, LANES), jnp.bfloat16) for n in (1, 2, 2)],
        in_specs=[VMEM] * len(sources),
        out_specs=[VMEM] * 3,
        compiler_params=LIMIT,
        name="near_merge",
    )(*partials)
    taken = swapped(across)
    pair_six, pair_thirteen = joined([ahead, taken], ((0, 0), (1, 0)), ((0, 1), (1, 1)))
    thirteen = shift_from(pair_thirteen, -FAR[2])
    six = shift_from(pair_six, -FAR[1])
    crossing = swapped(joined([six, thirteen], ((0, 1), (1, 1))))
    arrived = [home, six, thirteen, crossing]
    blocks = ((0, 0), (1, 0), (2, 0), (3, 0), (3, 1))
    return pl.pallas_call(
        lambda *refs: far_merge_kernel(blocks, *refs),
        out_shape=jax.ShapeDtypeStruct((1, heads, latent_width), jnp.bfloat16),
        in_specs=[VMEM] * len(arrived),
        out_specs=VMEM,
        compiler_params=LIMIT,
        name="far_merge",
    )(*arrived)


def solution(mesh):
    return jax.shard_map(
        local,
        mesh=mesh,
        in_specs=(
            P(("groups", "seq"), "head", None),
            P(("groups", "seq"), "head"),
            P(("groups", "seq", "head"), None, None),
            P(("groups", "seq", "head"), None),
            P("groups", None),
            P("groups"),
        ),
        out_specs=P(("groups", "seq"), "head", None),
        check_vma=False,
    )
```
